32 devices in a mesh: m: 2 (over x), kk: 4 (over z), g: 4 (over y, core).
Axes of the slice: x: 2, y: 2, z: 4, core: 2. Of those that a mesh axis runs over, the one named last changes fastest.
Arguments:
- a_mat: bfloat16 [6144, 8192], P(('m', 'g'), 'kk'), parts along dimension 0
Outputs:
- output: float32 [8, 3, 768, 768], P(('m', 'g'), None, 'kk'), parts along dimension 0
There are 2 independent parts. The reference program is written for one: setup_inputs(seed, part) draws one part's arguments, and reference() takes and returns one part's arrays. A program takes and returns all parts, laid end to end along the dimension named above; each array names one.
All inputs are finite; a program needn't handle non-finite values.
Results may differ from the reference program's by a relative error of at most 0.001.
Values are sent between devices in bfloat16 or wider.
A program may use at most 1 GiB of HBM per device.

```python
import math
import jax
import jax.numpy as jnp
from jax import lax

N_ROWS = 3072
K_COLS = 8192
GROUP_SIZE = 4

BLOCK_ROWS = N_ROWS // GROUP_SIZE
SLOT_COUNT = GROUP_SIZE // 2 + 1


def pair_table(groups):
    half_size = groups // 2
    step_width = max(1, math.isqrt(half_size))
    left_tab = []
    right_tab = []
    for dev_pos in range(groups):
        left_tab.append(dev_pos)
        right_tab.append(dev_pos)
        for diff_pos in range(1, half_size + 1):
            big_off = -(-diff_pos // step_width) * step_width
            if 2 * diff_pos == groups and dev_pos >= half_size:
                left_tab.append(-1)
                right_tab.append(-1)
            else:
                left_tab.append((dev_pos + big_off) % groups)
                right_tab.append((dev_pos + big_off - diff_pos) % groups)
    return left_tab, right_tab


def setup_inputs(seed: int = 0, part: int = 0) -> dict:
    base_key = jax.random.fold_in(jax.random.key(seed), part)
    key_val, key_scale = jax.random.split(base_key)
    values = jax.random.normal(key_val, (GROUP_SIZE, BLOCK_ROWS, K_COLS), jnp.float32)
    block_scale = jax.random.uniform(key_scale, (GROUP_SIZE, 1, 1), jnp.float32, 0.7, 1.4)
    a_mat = (values * block_scale).reshape(N_ROWS, K_COLS) * (K_COLS ** -0.25)
    return {"a_mat": a_mat.astype(jnp.bfloat16)}


def reference(a_mat):
    left_tab, right_tab = pair_table(GROUP_SIZE)
    pair_idx = jnp.array([[max(left_val, 0), max(right_val, 0)] for left_val, right_val in zip(left_tab, right_tab)], dtype=jnp.int32)
    keep_slot = jnp.array([left_val >= 0 for left_val in left_tab])
    blocks = a_mat.reshape(GROUP_SIZE, BLOCK_ROWS, K_COLS)

    def one_block(pair_row):
        row_blk = lax.dynamic_index_in_dim(blocks, pair_row[0], 0, keepdims=False)
        col_blk = lax.dynamic_index_in_dim(blocks, pair_row[1], 0, keepdims=False)
        return jnp.dot(row_blk, col_blk.T, preferred_element_type=jnp.float32)

    products = lax.map(one_block, pair_idx)
    products = jnp.where(keep_slot[:, None, None], products, 0.0)
    return products.reshape(GROUP_SIZE, SLOT_COUNT, BLOCK_ROWS, BLOCK_ROWS)
```

```python
import jax
import jax.numpy as jnp
from jax import lax
from jax.experimental import pallas as pl
from jax.experimental.pallas import tpu as pltpu
from jax.sharding import PartitionSpec as P

MESH = pl.DeviceIdType.MESH
NZ = 4
NG = 4


def kernel(a_hbm, out_hbm, abuf, part, ring, fin, load_sem, a_send, a_recv, f_send,
           z_send, z_recv, t_send, t_recv, o_sem):
    z = lax.axis_index("kk")
    g = lax.axis_index("g")
    rows = a_hbm.shape[0]
    qr = rows // NZ
    side = z // 2
    inner = ((z + 1) // 2) % 2
    has3 = ((g + 1) // 2) % 2
    toward = z + 1 - 2 * side
    away = z - 1 + 2 * side

    def mirror(q):
        return q + side * (3 - 2 * q)

    def order(i):
        return mirror(3 - i + inner * (i // 2) * (2 * i - 5))

    bar = pltpu.get_barrier_semaphore()
    for d in range(1, NG):
        pl.semaphore_signal(bar, inc=1, device_id={"g": (g + d) % NG}, device_id_type=MESH)
    pl.semaphore_signal(bar, inc=1, device_id={"kk": toward}, device_id_type=MESH)

    @pl.when(inner == 1)
    def _():
        pl.semaphore_signal(bar, inc=1, device_id={"kk": away}, device_id_type=MESH)

    load = pltpu.make_async_copy(a_hbm, abuf.at[0], load_sem)
    load.start()
    pl.semaphore_wait(bar, NG + inner)

    def chunk(q):
        return pl.ds(pl.multiple_of(q * qr, qr), qr)

    own_slot = 1 + g // 3

    def own_copy(q):
        return pltpu.make_async_remote_copy(
            a_hbm.at[chunk(q)], abuf.at[own_slot, chunk(q)], a_send.at[q], a_recv.at[own_slot - 1, q],
            device_id={"g": (g + NG - 1) % NG}, device_id_type=MESH)

    def arrival(slot, q):
        return pltpu.make_async_remote_copy(
            a_hbm.at[chunk(q)], abuf.at[slot, chunk(q)], a_send.at[q], a_recv.at[slot - 1, q],
            device_id={"g": (g + NG - 1) % NG}, device_id_type=MESH)

    fwd_slot = 4 - g

    def forward(q):
        s = jnp.clip(fwd_slot, 1, 2)
        return pltpu.make_async_remote_copy(
            abuf.at[s, chunk(q)], abuf.at[s, chunk(q)], f_send.at[q], a_recv.at[s - 1, q],
            device_id={"g": (g + NG - 1) % NG}, device_id_type=MESH)

    @pl.loop(0, NZ)
    def _(i):
        own_copy(order(i)).start()

    def product(b, q):
        if b == 0:
            left, right = 0, 0
        elif b == 1:
            two = (g // 2) * (1 - g % 2)
            left, right = 1 - two, two
        else:
            left, right = 2, 0
        part[b, q] = lax.dot_general(abuf[left, chunk(q)], abuf[right], (((1,), (1,)), ((), ())),
                                     preferred_element_type=jnp.float32)

    def z_copy(src, d, b, q, dev):
        return pltpu.make_async_remote_copy(
            src, ring.at[d, b, q], z_send.at[d, b, q], z_recv.at[d, b, q],
            device_id={"kk": dev}, device_id_type=MESH)

    def compute(b):
        if b == 1:
            @pl.when(g == 2)
            def _():
                for q in range(NZ):
                    arrival(1, q).wait_recv()

        @pl.loop(0, NZ)
        def _(i):
            q = order(i)
            if b == 1:
                @pl.when(g != 2)
                def _():
                    arrival(1, q).wait_recv()

                @pl.when(g == 3)
                def _():
                    forward(q).start()
            if b == 2:
                @pl.when(g == 1)
                def _():
                    arrival(2, q).wait_recv()
            product(b, q)

            @pl.when((inner == 0) & (i < 3))
            def _():
                z_copy(part.at[b, q], side, b, q, toward).start()

    def add_in(d, b, q):
        @pl.loop(0, qr // 16)
        def _(r):
            rs = pl.ds(pl.multiple_of(r * 16, 16), 16)
            ring[d, b, q, rs] = ring[d, b, q, rs] + part[b, q, rs]

    def wait_in(d, b, q):
        z_copy(ring.at[d, b, q], d, b, q, toward).wait_recv()

    def group1(b):
        @pl.when(inner == 1)
        def _():
            for mq in (3, 2):
                q = mirror(mq)
                wait_in(side, b, q)
                add_in(side, b, q)
                z_copy(ring.at[side, b, q], side, b, q, toward).start()
            q = mirror(0)
            wait_in(1 - side, b, q)
            add_in(1 - side, b, q)
            z_copy(ring.at[1 - side, b, q], 1 - side, b, q, away).start()

    def final(d, b, q):
        @pl.loop(0, qr // 16)
        def _(r):
            rs = pl.ds(pl.multiple_of(r * 16, 16), 16)
            fin[b, rs] = ring[d, b, q, rs] + part[b, q, rs]

    def out_copy(src, slot):
        return pltpu.make_async_copy(fin.at[src], out_hbm.at[slot], o_sem.at[slot])

    def hand_over():
        return pltpu.make_async_remote_copy(
            fin.at[1], fin.at[2], t_send, t_recv, device_id={"g": (g + 2) % NG}, device_id_type=MESH)

    def group2(b):
        @pl.when(inner == 1)
        def _():
            q = mirror(1)
            wait_in(side, b, q)
            add_in(side, b, q)
            wait_in(1 - side, b, q)

            @pl.loop(0, qr // 16)
            def _(r):
                rs = pl.ds(pl.multiple_of(r * 16, 16), 16)
                fin[b, rs] = ring[1 - side, b, q, rs] + ring[side, b, q, rs]

        @pl.when(inner == 0)
        def _():
            q = mirror(0)
            wait_in(1 - side, b, q)
            final(1 - side, b, q)

        if b == 0:
            out_copy(0, 0).start()
        elif b == 1:
            @pl.when(g != 2)
            def _():
                out_copy(1, 1).start()

            @pl.when(g == 2)
            def _():
                hand_over().start()
        else:
            out_copy(2, 3 - g).start()

    load.wait()
    compute(0)

    @pl.when(g >= 2)
    def _():
        @pl.loop(0, qr // 16)
        def _(r):
            fin[3, pl.ds(pl.multiple_of(r * 16, 16), 16)] = jnp.zeros((16, rows), jnp.float32)
        out_copy(3, 2).start()

    @pl.when(g == 2)
    def _():
        @pl.loop(0, NZ)
        def _(i):
            q = order(i)
            arrival(2, q).wait_recv()
            forward(q).start()

    group1(0)
    compute(1)
    group2(0)
    group1(1)

    @pl.when(has3 == 1)
    def _():
        compute(2)

    group2(1)

    @pl.when(has3 == 1)
    def _():
        group1(2)
        group2(2)

    @pl.when(g == 0)
    def _():
        hand_over().wait_recv()
        out_copy(2, 2).start()

    @pl.loop(0, NZ)
    def _(q):
        own_copy(q).wait_send()

    @pl.when(g >= 2)
    def _():
        @pl.loop(0, NZ)
        def _(q):
            forward(q).wait_send()

    @pl.when(g == 2)
    def _():
        hand_over().wait_send()

    def drain(b):
        @pl.when(inner == 0)
        def _():
            for mq in (3, 2, 1):
                q = mirror(mq)
                z_copy(part.at[b, q], side, b, q, toward).wait_send()

        @pl.when(inner == 1)
        def _():
            for mq in (3, 2):
                q = mirror(mq)
                z_copy(ring.at[side, b, q], side, b, q, toward).wait_send()
            q = mirror(0)
            z_copy(ring.at[1 - side, b, q], 1 - side, b, q, away).wait_send()

    drain(0)
    drain(1)

    @pl.when(has3 == 1)
    def _():
        drain(2)

    for s in range(3):
        out_copy(s, s).wait()


def solution(mesh):
    def local_fn(a_blk):
        rows, cols = a_blk.shape
        qr = rows // NZ
        dma = pltpu.SemaphoreType.DMA
        out = pl.pallas_call(
            kernel,
            out_shape=jax.ShapeDtypeStruct((3, qr, rows), jnp.float32),
            in_specs=[pl.BlockSpec(memory_space=pl.ANY)],
            out_specs=pl.BlockSpec(memory_space=pl.ANY),
            scratch_shapes=[
                pltpu.VMEM((3, rows, cols), jnp.bfloat16),
                pltpu.VMEM((3, NZ, qr, rows), jnp.float32),
                pltpu.VMEM((2, 3, NZ, qr, rows), jnp.float32),
                pltpu.VMEM((4, qr, rows), jnp.float32),
                dma, dma((NZ,)), dma((2, NZ)), dma((NZ,)),
                dma((2, 3, NZ)), dma((2, 3, NZ)), dma, dma, dma((3,)),
            ],
            compiler_params=pltpu.CompilerParams(
                collective_id=0, has_side_effects=True, vmem_limit_bytes=56 * 2**20),
        )(a_blk)
        return out[None]

    return jax.shard_map(local_fn, mesh=mesh, in_specs=(P(("m", "g"), "kk"),),
                         out_specs=P(("m", "g"), None, "kk", None), check_vma=False)
```

```python
import jax
import jax.numpy as jnp
from jax import lax
from jax.experimental import pallas as pl
from jax.experimental.pallas import tpu as pltpu
from jax.sharding import PartitionSpec as P

MESH = pl.DeviceIdType.MESH
NZ = 4
NG = 4
SENT = {3: 768, 2: 640, 1: 384}


def kernel(a_hbm, out_hbm, abuf, part, ring, fin, load_sem, a_send, a_recv, f_send,
           z_send, z_recv, t_send, t_recv, o_sem):
    z = lax.axis_index("kk")
    g = lax.axis_index("g")
    rows = a_hbm.shape[0]
    qr = rows // NZ
    side = z // 2
    inner = ((z + 1) // 2) % 2
    has3 = ((g + 1) // 2) % 2
    toward = z + 1 - 2 * side
    away = z - 1 + 2 * side

    def mirror(q):
        return q + side * (3 - 2 * q)

    def order(i):
        return mirror(3 - i + inner * (i // 2) * (2 * i - 5))

    bar = pltpu.get_barrier_semaphore()
    for d in range(1, NG):
        pl.semaphore_signal(bar, inc=1, device_id={"g": (g + d) % NG}, device_id_type=MESH)
    pl.semaphore_signal(bar, inc=1, device_id={"kk": toward}, device_id_type=MESH)

    @pl.when(inner == 1)
    def _():
        pl.semaphore_signal(bar, inc=1, device_id={"kk": away}, device_id_type=MESH)

    load = pltpu.make_async_copy(a_hbm, abuf.at[0], load_sem)
    load.start()
    pl.semaphore_wait(bar, NG + inner)

    def chunk(q):
        return pl.ds(pl.multiple_of(q * qr, qr), qr)

    own_slot = 1 + g // 3

    def own_copy(q):
        return pltpu.make_async_remote_copy(
            a_hbm.at[chunk(q)], abuf.at[own_slot, chunk(q)], a_send.at[q], a_recv.at[own_slot - 1, q],
            device_id={"g": (g + NG - 1) % NG}, device_id_type=MESH)

    def arrival(slot, q):
        return pltpu.make_async_remote_copy(
            a_hbm.at[chunk(q)], abuf.at[slot, chunk(q)], a_send.at[q], a_recv.at[slot - 1, q],
            device_id={"g": (g + NG - 1) % NG}, device_id_type=MESH)

    fwd_slot = 4 - g

    def forward(q):
        s = jnp.clip(fwd_slot, 1, 2)
        return pltpu.make_async_remote_copy(
            abuf.at[s, chunk(q)], abuf.at[s, chunk(q)], f_send.at[q], a_recv.at[s - 1, q],
            device_id={"g": (g + NG - 1) % NG}, device_id_type=MESH)

    @pl.loop(0, NZ)
    def _(i):
        own_copy(order(i)).start()

    def product(b, q):
        if b == 0:
            left, right = 0, 0
        elif b == 1:
            two = (g // 2) * (1 - g % 2)
            left, right = 1 - two, two
        else:
            left, right = 2, 0
        part[b, q] = lax.dot_general(abuf[left, chunk(q)], abuf[right], (((1,), (1,)), ((), ())),
                                     preferred_element_type=jnp.float32)

    half = qr // 2

    def part_of(b, d, mq, h):
        rs = pl.ds(h * half, half)
        size = rows if b else SENT[mq]
        start = d * (rows - size)
        return rs, pl.ds(pl.multiple_of(start, 128), size)

    def z_copy(src, b, d, mq, q, h, dev):
        rs, cs = part_of(b, d, mq, h)
        return pltpu.make_async_remote_copy(
            src.at[q, rs, cs], ring.at[d, b, q, rs, cs],
            z_send.at[d, b, q, h], z_recv.at[d, b, q, h],
            device_id={"kk": dev}, device_id_type=MESH)

    def near_send(src, b, mq, h):
        return z_copy(src, b, side, mq, mirror(mq), h, toward)

    def far_send(b, h):
        return z_copy(ring.at[1 - side, b], b, 1 - side, 3, mirror(0), h, away)

    def wait_near(b, mq, h):
        near_send(ring.at[side, b], b, mq, h).wait_recv()

    def wait_far(b, mq, h):
        d = 1 - side
        z_copy(ring.at[d, b], b, d, 3 - mq, mirror(mq), h, toward).wait_recv()

    def compute(b):
        if b == 1:
            @pl.when(g == 2)
            def _():
                for q in range(NZ):
                    arrival(1, q).wait_recv()

        @pl.loop(0, NZ)
        def _(i):
            q = order(i)
            if b == 1:
                @pl.when(g != 2)
                def _():
                    arrival(1, q).wait_recv()

                @pl.when(g == 3)
                def _():
                    forward(q).start()
            if b == 2:
                @pl.when(g == 1)
                def _():
                    arrival(2, q).wait_recv()
            product(b, q)

            for k in range(3):
                @pl.when((inner == 0) & (i == k))
                def _():
                    for h in range(2):
                        near_send(part.at[b], b, 3 - k, h).start()

    def add_in(b, d, mq, q, h):
        _, cs = part_of(b, d, mq, h)

        @pl.loop(0, half // 16)
        def _(r):
            rs = pl.ds(pl.multiple_of(h * half + r * 16, 16), 16)
            ring[d, b, q, rs, cs] = ring[d, b, q, rs, cs] + part[b, q, rs, cs]

    def group1(b):
        @pl.when(inner == 1)
        def _():
            for mq, h in ((3, 0), (3, 1), (0, 0), (2, 0), (0, 1), (2, 1)):
                if mq:
                    wait_near(b, mq, h)
                    add_in(b, side, mq, mirror(mq), h)
                    near_send(ring.at[side, b], b, mq, h).start()
                else:
                    wait_far(b, 0, h)
                    add_in(b, 1 - side, 3, mirror(0), h)
                    far_send(b, h).start()

    def out_copy(src, slot):
        return pltpu.make_async_copy(fin.at[src], out_hbm.at[slot], o_sem.at[slot])

    def hand_over():
        return pltpu.make_async_remote_copy(
            fin.at[1], fin.at[2], t_send, t_recv, device_id={"g": (g + 2) % NG}, device_id_type=MESH)

    def group2(b):
        @pl.when(inner == 1)
        def _():
            q = mirror(1)
            for h in range(2):
                wait_far(b, 1, h)
                wait_near(b, 1, h)
                if b:
                    @pl.loop(0, half // 16)
                    def _(r):
                        rs = pl.ds(pl.multiple_of(h * half + r * 16, 16), 16)
                        fin[b, rs] = ring[0, b, q, rs] + part[b, q, rs] + ring[1, b, q, rs]

        if b == 0:
            one, mid = SENT[2], SENT[1]
            lo = rows - one

            @pl.when(z == 1)
            def _():
                turned = ring[1, 0, 0, 0:lo, lo:mid].T
                fin[0, :, 0:lo] = ring[0, 0, 1, :, 0:lo] + turned[mid - lo - qr:]
                fin[0, :, lo:mid] = ring[0, 0, 1, :, lo:mid] + part[0, 1, :, lo:mid] + ring[1, 0, 1, :, lo:mid]
                turned = jnp.concatenate([ring[0, 0, 2, :, lo:mid], ring[0, 0, 3, :, lo:mid]], axis=0).T
                fin[0, :, mid:] = ring[1, 0, 1, :, mid:] + turned[mid - lo - qr:]

            @pl.when(z == 2)
            def _():
                turned = ring[0, 0, 3, qr - lo:, mid:one].T
                fin[0, :, one:] = ring[1, 0, 2, :, one:] + turned[:qr]
                fin[0, :, mid:one] = ring[0, 0, 2, :, mid:one] + part[0, 2, :, mid:one] + ring[1, 0, 2, :, mid:one]
                turned = jnp.concatenate([ring[1, 0, 0, :, mid:one], ring[1, 0, 1, :, mid:one]], axis=0).T
                fin[0, :, :mid] = ring[0, 0, 2, :, :mid] + turned[:qr]

        @pl.when(inner == 0)
        def _():
            q = mirror(0)
            for h in range(2):
                wait_far(b, 0, h)

                @pl.loop(0, half // 16)
                def _(r):
                    rs = pl.ds(pl.multiple_of(h * half + r * 16, 16), 16)
                    fin[b, rs] = ring[1 - side, b, q, rs] + part[b, q, rs]

        if b == 0:
            out_copy(0, 0).start()
        elif b == 1:
            @pl.when(g != 2)
            def _():
                out_copy(1, 1).start()

            @pl.when(g == 2)
            def _():
                hand_over().start()
        else:
            out_copy(2, 3 - g).start()

    load.wait()
    compute(0)

    @pl.when(g >= 2)
    def _():
        @pl.loop(0, qr // 16)
        def _(r):
            fin[3, pl.ds(pl.multiple_of(r * 16, 16), 16)] = jnp.zeros((16, rows), jnp.float32)
        out_copy(3, 2).start()

    @pl.when(g == 2)
    def _():
        @pl.loop(0, NZ)
        def _(i):
            q = order(i)
            arrival(2, q).wait_recv()
            forward(q).start()

    group1(0)
    compute(1)
    group2(0)
    group1(1)

    @pl.when(has3 == 1)
    def _():
        compute(2)

    group2(1)

    @pl.when(has3 == 1)
    def _():
        group1(2)
        group2(2)

    @pl.when(g == 0)
    def _():
        hand_over().wait_recv()
        out_copy(2, 2).start()

    @pl.loop(0, NZ)
    def _(q):
        own_copy(q).wait_send()

    @pl.when(g >= 2)
    def _():
        @pl.loop(0, NZ)
        def _(q):
            forward(q).wait_send()

    @pl.when(g == 2)
    def _():
        hand_over().wait_send()

    def drain(b):
        for h in range(2):
            @pl.when(inner == 0)
            def _():
                for mq in (3, 2, 1):
                    near_send(part.at[b], b, mq, h).wait_send()

            @pl.when(inner == 1)
            def _():
                for mq in (3, 2):
                    near_send(ring.at[side, b], b, mq, h).wait_send()
                far_send(b, h).wait_send()

    drain(0)
    drain(1)

    @pl.when(has3 == 1)
    def _():
        drain(2)

    for s in range(3):
        out_copy(s, s).wait()


def solution(mesh):
    def local_fn(a_blk):
        rows, cols = a_blk.shape
        qr = rows // NZ
        dma = pltpu.SemaphoreType.DMA
        out = pl.pallas_call(
            kernel,
            out_shape=jax.ShapeDtypeStruct((3, qr, rows), jnp.float32),
            in_specs=[pl.BlockSpec(memory_space=pl.ANY)],
            out_specs=pl.BlockSpec(memory_space=pl.ANY),
            scratch_shapes=[
                pltpu.VMEM((3, rows, cols), jnp.bfloat16),
                pltpu.VMEM((3, NZ, qr, rows), jnp.float32),
                pltpu.VMEM((2, 3, NZ, qr, rows), jnp.float32),
                pltpu.VMEM((4, qr, rows), jnp.float32),
                dma, dma((NZ,)), dma((2, NZ)), dma((NZ,)),
                dma((2, 3, NZ, 2)), dma((2, 3, NZ, 2)), dma, dma, dma((3,)),
            ],
            compiler_params=pltpu.CompilerParams(
                collective_id=0, has_side_effects=True, vmem_limit_bytes=56 * 2**20),
        )(a_blk)
        return out[None]

    return jax.shard_map(local_fn, mesh=mesh, in_specs=(P(("m", "g"), "kk"),),
                         out_specs=P(("m", "g"), None, "kk", None), check_vma=False)
```

```python
import jax
import jax.numpy as jnp
from jax import lax
from jax.experimental import pallas as pl
from jax.experimental.pallas import tpu as pltpu
from jax.sharding import PartitionSpec as P

MESH = pl.DeviceIdType.MESH
NZ = 4
NG = 4
SENT = {3: 768, 2: 640, 1: 384}


def kernel(a_hbm, out, abuf, part, ring, got, load_sem, a_send, a_recv, f_send,
           z_send, z_recv, t_send, t_recv):
    z = lax.axis_index("kk")
    g = lax.axis_index("g")
    rows = a_hbm.shape[0]
    qr = rows // NZ
    side = z // 2
    inner = ((z + 1) // 2) % 2
    has3 = ((g + 1) // 2) % 2
    toward = z + 1 - 2 * side
    away = z - 1 + 2 * side

    def mirror(q):
        return q + side * (3 - 2 * q)

    def order(i):
        return mirror(3 - i + inner * (i // 2) * (2 * i - 5))

    bar = pltpu.get_barrier_semaphore()
    for d in range(1, NG):
        pl.semaphore_signal(bar, inc=1, device_id={"g": (g + d) % NG}, device_id_type=MESH)
    pl.semaphore_signal(bar, inc=1, device_id={"kk": toward}, device_id_type=MESH)

    @pl.when(inner == 1)
    def _():
        pl.semaphore_signal(bar, inc=1, device_id={"kk": away}, device_id_type=MESH)

    load = pltpu.make_async_copy(a_hbm, abuf.at[0], load_sem)
    load.start()
    pl.semaphore_wait(bar, NG + inner)

    def chunk(q):
        return pl.ds(pl.multiple_of(q * qr, qr), qr)

    own_slot = 1 + g // 3

    def own_copy(q):
        return pltpu.make_async_remote_copy(
            a_hbm.at[chunk(q)], abuf.at[own_slot, chunk(q)], a_send.at[q], a_recv.at[own_slot - 1, q],
            device_id={"g": (g + NG - 1) % NG}, device_id_type=MESH)

    def arrival(slot, q):
        return pltpu.make_async_remote_copy(
            a_hbm.at[chunk(q)], abuf.at[slot, chunk(q)], a_send.at[q], a_recv.at[slot - 1, q],
            device_id={"g": (g + NG - 1) % NG}, device_id_type=MESH)

    fwd_slot = 4 - g

    def forward(q):
        s = jnp.clip(fwd_slot, 1, 2)
        return pltpu.make_async_remote_copy(
            abuf.at[s, chunk(q)], abuf.at[s, chunk(q)], f_send.at[q], a_recv.at[s - 1, q],
            device_id={"g": (g + NG - 1) % NG}, device_id_type=MESH)

    @pl.loop(0, NZ)
    def _(i):
        own_copy(order(i)).start()

    def product(b, q):
        if b == 0:
            left, right = 0, 0
        elif b == 1:
            two = (g // 2) * (1 - g % 2)
            left, right = 1 - two, two
        else:
            left, right = 2, 0
        part[b, q] = lax.dot_general(abuf[left, chunk(q)], abuf[right], (((1,), (1,)), ((), ())),
                                     preferred_element_type=jnp.float32)

    half = qr // 2

    def part_of(b, d, mq, h):
        rs = pl.ds(h * half, half)
        size = rows if b else SENT[mq]
        start = d * (rows - size)
        return rs, pl.ds(pl.multiple_of(start, 128), size)

    def z_copy(src, b, d, mq, q, h, dev):
        rs, cs = part_of(b, d, mq, h)
        return pltpu.make_async_remote_copy(
            src.at[q, rs, cs], ring.at[d, b, q, rs, cs],
            z_send.at[d, b, q, h], z_recv.at[d, b, q, h],
            device_id={"kk": dev}, device_id_type=MESH)

    def near_send(src, b, mq, h):
        return z_copy(src, b, side, mq, mirror(mq), h, toward)

    def far_send(b, h):
        return z_copy(ring.at[1 - side, b], b, 1 - side, 3, mirror(0), h, away)

    def wait_near(b, mq, h):
        near_send(ring.at[side, b], b, mq, h).wait_recv()

    def wait_far(b, mq, h):
        d = 1 - side
        z_copy(ring.at[d, b], b, d, 3 - mq, mirror(mq), h, toward).wait_recv()

    def compute(b):
        if b == 1:
            @pl.when(g == 2)
            def _():
                for q in range(NZ):
                    arrival(1, q).wait_recv()

        @pl.loop(0, NZ)
        def _(i):
            q = order(i)
            if b == 1:
                @pl.when(g != 2)
                def _():
                    arrival(1, q).wait_recv()

                @pl.when(g == 3)
                def _():
                    forward(q).start()
            if b == 2:
                @pl.when(g == 1)
                def _():
                    arrival(2, q).wait_recv()
            product(b, q)

            for k in range(3):
                @pl.when((inner == 0) & (i == k))
                def _():
                    for h in range(2):
                        near_send(part.at[b], b, 3 - k, h).start()

    def add_in(b, d, mq, q, h):
        _, cs = part_of(b, d, mq, h)

        @pl.loop(0, half // 16)
        def _(r):
            rs = pl.ds(pl.multiple_of(h * half + r * 16, 16), 16)
            ring[d, b, q, rs, cs] = ring[d, b, q, rs, cs] + part[b, q, rs, cs]

    def group1(b):
        @pl.when(inner == 1)
        def _():
            for mq, h in ((3, 0), (3, 1), (0, 0), (2, 0), (0, 1), (2, 1)):
                if mq:
                    wait_near(b, mq, h)
                    add_in(b, side, mq, mirror(mq), h)
                    near_send(ring.at[side, b], b, mq, h).start()
                else:
                    wait_far(b, 0, h)
                    add_in(b, 1 - side, 3, mirror(0), h)
                    far_send(b, h).start()

    def hand_over():
        return pltpu.make_async_remote_copy(
            out.at[2], got, t_send, t_recv, device_id={"g": (g + 2) % NG}, device_id_type=MESH)

    def group2(b):
        two = (g // 2) * (1 - g % 2)
        slot = (0, 1 + two, 3 - g)[b]

        @pl.when(inner == 1)
        def _():
            q = mirror(1)
            for h in range(2):
                wait_far(b, 1, h)
                wait_near(b, 1, h)
                if b:
                    @pl.loop(0, half // 16)
                    def _(r):
                        rs = pl.ds(pl.multiple_of(h * half + r * 16, 16), 16)
                        out[slot, rs] = ring[0, b, q, rs] + part[b, q, rs] + ring[1, b, q, rs]

        if b == 0:
            one, mid = SENT[2], SENT[1]
            lo = rows - one

            @pl.when(z == 1)
            def _():
                turned = ring[1, 0, 0, 0:lo, lo:mid].T
                out[0, :, 0:lo] = ring[0, 0, 1, :, 0:lo] + turned[mid - lo - qr:]
                out[0, :, lo:mid] = ring[0, 0, 1, :, lo:mid] + part[0, 1, :, lo:mid] + ring[1, 0, 1, :, lo:mid]
                turned = jnp.concatenate([ring[0, 0, 2, :, lo:mid], ring[0, 0, 3, :, lo:mid]], axis=0).T
                out[0, :, mid:] = ring[1, 0, 1, :, mid:] + turned[mid - lo - qr:]

            @pl.when(z == 2)
            def _():
                turned = ring[0, 0, 3, qr - lo:, mid:one].T
                out[0, :, one:] = ring[1, 0, 2, :, one:] + turned[:qr]
                out[0, :, mid:one] = ring[0, 0, 2, :, mid:one] + part[0, 2, :, mid:one] + ring[1, 0, 2, :, mid:one]
                turned = jnp.concatenate([ring[1, 0, 0, :, mid:one], ring[1, 0, 1, :, mid:one]], axis=0).T
                out[0, :, :mid] = ring[0, 0, 2, :, :mid] + turned[:qr]

        @pl.when(inner == 0)
        def _():
            q = mirror(0)
            for h in range(2):
                wait_far(b, 0, h)

                @pl.loop(0, half // 16)
                def _(r):
                    rs = pl.ds(pl.multiple_of(h * half + r * 16, 16), 16)
                    out[slot, rs] = ring[1 - side, b, q, rs] + part[b, q, rs]

        if b == 1:
            @pl.when(g == 2)
            def _():
                hand_over().start()

    def fill(value):
        @pl.loop(0, qr // 16)
        def _(r):
            rs = pl.ds(pl.multiple_of(r * 16, 16), 16)
            out[2, rs] = value(rs)

    load.wait()
    compute(0)

    @pl.when(g == 2)
    def _():
        @pl.loop(0, NZ)
        def _(i):
            q = order(i)
            arrival(2, q).wait_recv()
            forward(q).start()

    group1(0)
    compute(1)
    group2(0)
    group1(1)

    @pl.when(has3 == 1)
    def _():
        compute(2)

    group2(1)

    @pl.when(has3 == 1)
    def _():
        group1(2)
        group2(2)

    @pl.when(g == 0)
    def _():
        hand_over().wait_recv()
        fill(lambda rs: got[rs])

    @pl.loop(0, NZ)
    def _(q):
        own_copy(q).wait_send()

    @pl.when(g >= 2)
    def _():
        @pl.loop(0, NZ)
        def _(q):
            forward(q).wait_send()

    @pl.when(g == 2)
    def _():
        hand_over().wait_send()

    @pl.when(g >= 2)
    def _():
        fill(lambda rs: jnp.zeros((16, rows), jnp.float32))

    def drain(b):
        for h in range(2):
            @pl.when(inner == 0)
            def _():
                for mq in (3, 2, 1):
                    near_send(part.at[b], b, mq, h).wait_send()

            @pl.when(inner == 1)
            def _():
                for mq in (3, 2):
                    near_send(ring.at[side, b], b, mq, h).wait_send()
                far_send(b, h).wait_send()

    drain(0)
    drain(1)

    @pl.when(has3 == 1)
    def _():
        drain(2)


def solution(mesh):
    def local_fn(a_blk):
        rows, cols = a_blk.shape
        qr = rows // NZ
        dma = pltpu.SemaphoreType.DMA
        out = pl.pallas_call(
            kernel,
            out_shape=jax.ShapeDtypeStruct((3, qr, rows), jnp.float32),
            in_specs=[pl.BlockSpec(memory_space=pltpu.HBM)],
            out_specs=pl.BlockSpec(memory_space=pltpu.VMEM),
            scratch_shapes=[
                pltpu.VMEM((3, rows, cols), jnp.bfloat16),
                pltpu.VMEM((3, NZ, qr, rows), jnp.float32),
                pltpu.VMEM((2, 3, NZ, qr, rows), jnp.float32),
                pltpu.VMEM((qr, rows), jnp.float32),
                dma, dma((NZ,)), dma((2, NZ)), dma((NZ,)),
                dma((2, 3, NZ, 2)), dma((2, 3, NZ, 2)), dma, dma,
            ],
            compiler_params=pltpu.CompilerParams(
                collective_id=0, has_side_effects=True, vmem_limit_bytes=50 * 2**20),
        )(a_blk)
        return out[None]

    return jax.shard_map(local_fn, mesh=mesh, in_specs=(P(("m", "g"), "kk"),),
                         out_specs=P(("m", "g"), None, "kk", None), check_vma=False)
```

```python
import jax
import jax.numpy as jnp
from jax import lax
from jax.experimental import pallas as pl
from jax.experimental.pallas import tpu as pltpu
from jax.sharding import PartitionSpec as P

MESH = pl.DeviceIdType.MESH
NZ = 4
NG = 4
SENT = {3: 768, 2: 640, 1: 384}


def kernel(a_hbm, out, abuf, part, ring, got, load_sem, a_send, u_send, f_send, a_recv,
           z_send, z_recv, t_send, t_recv):
    z = lax.axis_index("kk")
    g = lax.axis_index("g")
    rows = a_hbm.shape[0]
    qr = rows // NZ
    side = z // 2
    inner = ((z + 1) // 2) % 2
    has3 = g % 2
    last = g // 3
    toward = z + 1 - 2 * side
    away = z - 1 + 2 * side

    def mirror(q):
        return q + side * (3 - 2 * q)

    def order(i):
        return mirror(3 - i + inner * (i // 2) * (2 * i - 5))

    def third(k, d):
        return pl.ds(pl.multiple_of((2 - k + d * (2 * k - 2)) * (rows // 3), rows // 3), rows // 3)

    def load(k):
        return pltpu.make_async_copy(a_hbm.at[third(k, side)], abuf.at[0, third(k, side)], load_sem.at[k])

    for k in range(3):
        load(k).start()

    bar = pltpu.get_barrier_semaphore()
    for d in (1, NG - 1):
        pl.semaphore_signal(bar, inc=1, device_id={"g": (g + d) % NG}, device_id_type=MESH)
    pl.semaphore_signal(bar, inc=1, device_id={"kk": toward}, device_id_type=MESH)

    @pl.when(inner == 1)
    def _():
        pl.semaphore_signal(bar, inc=1, device_id={"kk": away}, device_id_type=MESH)

    def chunk(q):
        return pl.ds(pl.multiple_of(q * qr, qr), qr)

    def row_copy(src, slot, q, d, send):
        return pltpu.make_async_remote_copy(
            src.at[chunk(q)], abuf.at[slot, chunk(q)], send.at[q], a_recv.at[slot - 1, q],
            device_id={"g": (g + d) % NG}, device_id_type=MESH)

    def own_copy(q):
        return row_copy(a_hbm, 1, q, NG - 1, a_send)

    def own_copy_up(q):
        return row_copy(a_hbm, 2, q, 1, u_send)

    def forward(q):
        return row_copy(abuf.at[1], 2, q, NG - 1, f_send)

    def arrival(slot, q):
        return row_copy(a_hbm, slot, q, NG - 1, a_send)

    def product(b, q):
        left = (0, 1 + last, 2 - last)[b]
        right = (0, last, 0)[b]
        part[b, q] = lax.dot_general(abuf[left, chunk(q)], abuf[right], (((1,), (1,)), ((), ())),
                                     preferred_element_type=jnp.float32)

    def product_third(q, k):
        load(k).wait()
        part[0, q, :, third(k, side)] = lax.dot_general(
            abuf[0, chunk(q)], abuf[0, third(k, side)], (((1,), (1,)), ((), ())),
            preferred_element_type=jnp.float32)

    half = qr // 2

    def pieces(b, mq):
        return 3 if b == 0 and mq == 3 else 2

    def part_of(b, d, mq, h):
        if pieces(b, mq) == 3:
            return pl.ds(0, qr), third(h, d)
        rs = pl.ds(h * half, half)
        size = rows if b else SENT[mq]
        start = d * (rows - size)
        return rs, pl.ds(pl.multiple_of(start, 128), size)

    def z_copy(src, b, d, mq, q, h, dev):
        rs, cs = part_of(b, d, mq, h)
        return pltpu.make_async_remote_copy(
            src.at[q, rs, cs], ring.at[d, b, q, rs, cs],
            z_send.at[d, b, q, h], z_recv.at[d, b, q, h],
            device_id={"kk": dev}, device_id_type=MESH)

    def near_send(src, b, mq, h):
        return z_copy(src, b, side, mq, mirror(mq), h, toward)

    def far_send(b, h):
        return z_copy(ring.at[1 - side, b], b, 1 - side, 3, mirror(0), h, away)

    def wait_near(b, mq, h):
        near_send(ring.at[side, b], b, mq, h).wait_recv()

    def wait_far(b, mq, h):
        d = 1 - side
        z_copy(ring.at[d, b], b, d, 3 - mq, mirror(mq), h, toward).wait_recv()

    def compute(b):
        def step(i):
            q = order(i)
            if b == 1:
                @pl.when(last == 0)
                def _():
                    arrival(1, q).wait_recv()

                @pl.when(g == 2)
                def _():
                    forward(q).start()

                @pl.when(last == 1)
                def _():
                    arrival(2, q).wait_recv()
            if b == 2:
                @pl.when(g == 1)
                def _():
                    arrival(2, q).wait_recv()
            product(b, q)
            for k in range(3):
                @pl.when((inner == 0) & (i == k))
                def _():
                    for h in range(pieces(b, 3 - k)):
                        near_send(part.at[b], b, 3 - k, h).start()

        if b == 1:
            @pl.when(last == 1)
            def _():
                for q in range(NZ):
                    arrival(1, q).wait_recv()
        pl.loop(0 if b else 1, NZ)(step)

    def start():
        q = order(0)
        for k in range(3):
            product_third(q, k)
            if k == 0:
                pl.semaphore_wait(bar, 3 + inner)

            @pl.when(inner == 0)
            def _():
                near_send(part.at[0], 0, 3, k).start()
            if k == 0:
                @pl.loop(0, NZ)
                def _(i):
                    own_copy(order(i)).start()

                @pl.when(g == 2)
                def _():
                    @pl.loop(0, NZ)
                    def _(i):
                        own_copy_up(order(i)).start()

    def row_loop(rs, body):
        @pl.loop(0, rs.size // 16)
        def _(r):
            body(pl.ds(pl.multiple_of(rs.start + r * 16, 16), 16))

    def add_in(b, d, mq, q, h):
        rs, cs = part_of(b, d, mq, h)

        def body(rr):
            ring[d, b, q, rr, cs] = ring[d, b, q, rr, cs] + part[b, q, rr, cs]
        row_loop(rs, body)

    def group1(b):
        if b == 0:
            turns = ((3, 0), (3, 1), (3, 2), (0, 0), (0, 1), (2, 0), (0, 2), (2, 1))
        else:
            turns = ((3, 0), (3, 1), (0, 0), (2, 0), (0, 1), (2, 1))

        @pl.when(inner == 1)
        def _():
            for mq, h in turns:
                if mq:
                    wait_near(b, mq, h)
                    add_in(b, side, mq, mirror(mq), h)
                    near_send(ring.at[side, b], b, mq, h).start()
                else:
                    wait_far(b, 0, h)
                    add_in(b, 1 - side, 3, mirror(0), h)
                    far_send(b, h).start()

    def hand_over():
        return pltpu.make_async_remote_copy(
            out.at[2], got, t_send, t_recv, device_id={"g": (g + 1) % NG}, device_id_type=MESH)

    def group2(b):
        slot = (0, 1 + last, (5 - g) // 2)[b]

        @pl.when(inner == 1)
        def _():
            q = mirror(1)
            for h in range(2):
                wait_far(b, 1, h)
                wait_near(b, 1, h)
                if b:
                    @pl.loop(0, half // 16)
                    def _(r):
                        rs = pl.ds(pl.multiple_of(h * half + r * 16, 16), 16)
                        out[slot, rs] = ring[0, b, q, rs] + part[b, q, rs] + ring[1, b, q, rs]

        if b == 0:
            one, mid = SENT[2], SENT[1]
            lo = rows - one

            @pl.when(z == 1)
            def _():
                turned = ring[1, 0, 0, 0:lo, lo:mid].T
                out[0, :, 0:lo] = ring[0, 0, 1, :, 0:lo] + turned[mid - lo - qr:]
                out[0, :, lo:mid] = ring[0, 0, 1, :, lo:mid] + part[0, 1, :, lo:mid] + ring[1, 0, 1, :, lo:mid]
                turned = jnp.concatenate([ring[0, 0, 2, :, lo:mid], ring[0, 0, 3, :, lo:mid]], axis=0).T
                out[0, :, mid:] = ring[1, 0, 1, :, mid:] + turned[mid - lo - qr:]

            @pl.when(z == 2)
            def _():
                turned = ring[0, 0, 3, qr - lo:, mid:one].T
                out[0, :, one:] = ring[1, 0, 2, :, one:] + turned[:qr]
                out[0, :, mid:one] = ring[0, 0, 2, :, mid:one] + part[0, 2, :, mid:one] + ring[1, 0, 2, :, mid:one]
                turned = jnp.concatenate([ring[1, 0, 0, :, mid:one], ring[1, 0, 1, :, mid:one]], axis=0).T
                out[0, :, :mid] = ring[0, 0, 2, :, :mid] + turned[:qr]

        @pl.when(inner == 0)
        def _():
            q = mirror(0)
            for h in range(pieces(b, 3)):
                wait_far(b, 0, h)
                rs, cs = part_of(b, 1 - side, 3, h)

                def body(rr):
                    out[slot, rr, cs] = ring[1 - side, b, q, rr, cs] + part[b, q, rr, cs]
                row_loop(rs, body)

        if b == 1:
            @pl.when(last == 1)
            def _():
                hand_over().start()

    def fill(value):
        @pl.loop(0, qr // 16)
        def _(r):
            rs = pl.ds(pl.multiple_of(r * 16, 16), 16)
            out[2, rs] = value(rs)

    start()
    compute(0)
    group1(0)
    compute(1)
    group2(0)
    group1(1)

    @pl.when(has3 == 1)
    def _():
        compute(2)

    group2(1)

    @pl.when(has3 == 1)
    def _():
        group1(2)
        group2(2)

    @pl.when(g == 0)
    def _():
        hand_over().wait_recv()
        fill(lambda rs: got[rs])

    @pl.loop(0, NZ)
    def _(q):
        own_copy(q).wait_send()

    @pl.when(g == 2)
    def _():
        @pl.loop(0, NZ)
        def _(q):
            own_copy_up(q).wait_send()
            forward(q).wait_send()

    @pl.when(last == 1)
    def _():
        hand_over().wait_send()

    @pl.when(g >= 2)
    def _():
        fill(lambda rs: jnp.zeros((16, rows), jnp.float32))

    def drain(b):
        @pl.when(inner == 0)
        def _():
            for mq in (3, 2, 1):
                for h in range(pieces(b, mq)):
                    near_send(part.at[b], b, mq, h).wait_send()

        @pl.when(inner == 1)
        def _():
            for mq in (3, 2):
                for h in range(pieces(b, mq)):
                    near_send(ring.at[side, b], b, mq, h).wait_send()
            for h in range(pieces(b, 3)):
                far_send(b, h).wait_send()

    drain(0)
    drain(1)

    @pl.when(has3 == 1)
    def _():
        drain(2)


def solution(mesh):
    def local_fn(a_blk):
        rows, cols = a_blk.shape
        qr = rows // NZ
        dma = pltpu.SemaphoreType.DMA
        out = pl.pallas_call(
            kernel,
            out_shape=jax.ShapeDtypeStruct((3, qr, rows), jnp.float32),
            in_specs=[pl.BlockSpec(memory_space=pltpu.HBM)],
            out_specs=pl.BlockSpec(memory_space=pltpu.VMEM),
            scratch_shapes=[
                pltpu.VMEM((3, rows, cols), jnp.bfloat16),
                pltpu.VMEM((3, NZ, qr, rows), jnp.float32),
                pltpu.VMEM((2, 3, NZ, qr, rows), jnp.float32),
                pltpu.VMEM((qr, rows), jnp.float32),
                dma((3,)), dma((NZ,)), dma((NZ,)), dma((NZ,)), dma((2, NZ)),
                dma((2, 3, NZ, 3)), dma((2, 3, NZ, 3)), dma, dma,
            ],
            compiler_params=pltpu.CompilerParams(
                collective_id=0, has_side_effects=True, vmem_limit_bytes=50 * 2**20),
        )(a_blk)
        return out[None]

    return jax.shard_map(local_fn, mesh=mesh, in_specs=(P(("m", "g"), "kk"),),
                         out_specs=P(("m", "g"), None, "kk", None), check_vma=False)
```

```python
import jax
import jax.numpy as jnp
from jax import lax
from jax.experimental import pallas as pl
from jax.experimental.pallas import tpu as pltpu
from jax.sharding import PartitionSpec as P

MESH = pl.DeviceIdType.MESH
NZ = 4
NG = 4
ROWS = 768
QR = ROWS // NZ
HALF = QR // 2
FIRST = 128
SENT = {3: 768, 2: 640, 1: 384}


def pieces(b, mq):
    return (1 if mq < 3 else 2) if b == 0 else 2


def near_index(b, mq, h):
    base = 0
    for k in range(b):
        base += sum(pieces(k, m) for m in (3, 2, 1)) + pieces(k, 3) + pieces(k, 2)
    return base + sum(pieces(b, m) for m in (3, 2, 1) if m > mq) + h


def far_index(b, mq, h):
    return near_index(b, 0, 0) + (pieces(b, 3) if mq else 0) + h


NRECV = near_index(3, 3, 0)


def kernel(a_hbm, out, abuf, part, ring, got, load_sem, a_send, a_recv, z_send, z_recv, t_send, t_recv):
    z = lax.axis_index("kk")
    g = lax.axis_index("g")
    side = z // 2
    inner = ((z + 1) // 2) % 2
    has3 = g % 2
    last = g // 3
    toward = z + 1 - 2 * side
    away = z - 1 + 2 * side

    def mirror(q):
        return q + side * (3 - 2 * q)

    def order(i):
        return mirror(3 - i + inner * (i // 2) * (2 * i - 5))

    def load(k):
        size = (QR, ROWS - QR)[k]
        start = ((1 - side) * (ROWS - QR), side * QR)[k]
        rs = pl.ds(pl.multiple_of(start, QR), size)
        return pltpu.make_async_copy(a_hbm.at[rs], abuf.at[0, rs], load_sem.at[k])

    load(0).start()
    load(1).start()

    bar = pltpu.get_barrier_semaphore()
    for d in (1, NG - 1):
        pl.semaphore_signal(bar, inc=1, device_id={"g": (g + d) % NG}, device_id_type=MESH)
    pl.semaphore_signal(bar, inc=1, device_id={"kk": toward}, device_id_type=MESH)

    @pl.when(inner == 1)
    def _():
        pl.semaphore_signal(bar, inc=1, device_id={"kk": away}, device_id_type=MESH)

    def chunk(q):
        return pl.ds(pl.multiple_of(q * QR, QR), QR)

    def row_copy(src, slot, q, d):
        return pltpu.make_async_remote_copy(
            src.at[chunk(q)], abuf.at[slot, chunk(q)], a_send, a_recv.at[slot - 1, q],
            device_id={"g": (g + d) % NG}, device_id_type=MESH)

    def arrival(slot, q):
        return row_copy(a_hbm, slot, q, NG - 1)

    def dot(x, y):
        return lax.dot_general(x, y, (((1,), (1,)), ((), ())), preferred_element_type=jnp.float32)

    def at(b, q, start, size):
        return pl.ds(pl.multiple_of(b * ROWS + q * QR + start, 16), size)

    def product(b, q):
        left = (0, 1 + last, 2 - last)[b]
        right = (0, last, 0)[b]
        part[at(b, q, 0, QR)] = dot(abuf[left, chunk(q)], abuf[right])

    def part_of(b, d, mq, h):
        if b:
            return h * HALF, HALF, pl.ds(0, ROWS)
        size = SENT[mq]
        start = d * (ROWS - size)
        if mq == 3:
            size = (FIRST, ROWS - FIRST)[h]
            start = ((1 - d) * (ROWS - FIRST), d * FIRST)[h]
        return 0, QR, pl.ds(pl.multiple_of(start, 128), size)

    def z_copy(src, b, d, mq, q, h, dev, index):
        start, size, cs = part_of(b, d, mq, h)
        return pltpu.make_async_remote_copy(
            src.at[at(b, q, start, size), cs], ring.at[d, at(b, q, start, size), cs],
            z_send, z_recv.at[index], device_id={"kk": dev}, device_id_type=MESH)

    def near_copy(src, b, mq, h, index):
        return z_copy(src, b, side, mq, mirror(mq), h, toward, index)

    def far_copy(b, mq, h):
        d = 1 - side
        return z_copy(ring.at[d], b, d, 3 - mq, mirror(mq), h, away, far_index(b, mq, h))

    def wait_near(b, mq, h):
        near_copy(part, b, mq, h, near_index(b, mq, h)).wait_recv()

    def wait_far(b, mq, h):
        far_copy(b, mq, h).wait_recv()

    def send_near(b, mq):
        for h in range(pieces(b, mq)):
            near_copy(part, b, mq, h, near_index(b, mq, h)).start()

    def start():
        q = order(0)
        cs = pl.ds(pl.multiple_of((1 - side) * (ROWS - FIRST), FIRST), FIRST)
        load(0).wait()
        part[at(0, q, 0, QR), cs] = dot(abuf[0, chunk(q)], abuf[0, cs])
        pl.semaphore_wait(bar, 3 + inner)

        @pl.when(inner == 0)
        def _():
            near_copy(part, 0, 3, 0, near_index(0, 3, 0)).start()

        @pl.loop(0, NZ)
        def _(i):
            row_copy(a_hbm, 1, order(i), NG - 1).start()

        @pl.when(g == 2)
        def _():
            @pl.loop(0, NZ)
            def _(i):
                row_copy(a_hbm, 2, order(i), 1).start()

        cs = pl.ds(pl.multiple_of(side * FIRST, FIRST), ROWS - FIRST)
        load(1).wait()
        part[at(0, q, 0, QR), cs] = dot(abuf[0, chunk(q)], abuf[0, cs])

        @pl.when(inner == 0)
        def _():
            near_copy(part, 0, 3, 1, near_index(0, 3, 1)).start()

    def compute(b):
        def step(i):
            q = order(i)
            if b == 1:
                @pl.when(last == 0)
                def _():
                    arrival(1, q).wait_recv()

                @pl.when(g == 2)
                def _():
                    row_copy(abuf.at[1], 2, q, NG - 1).start()

                @pl.when(last == 1)
                def _():
                    arrival(2, q).wait_recv()
            if b == 2:
                @pl.when(g == 1)
                def _():
                    arrival(2, q).wait_recv()
            product(b, q)
            for k in range(0 if b else 1, 3):
                @pl.when((inner == 0) & (i == k))
                def _():
                    send_near(b, 3 - k)

        if b == 1:
            @pl.when(last == 1)
            def _():
                for q in range(NZ):
                    arrival(1, q).wait_recv()
        pl.loop(0 if b else 1, NZ)(step)

    def row_loop(b, q, start, size, body):
        @pl.loop(0, size // 16)
        def _(r):
            body(at(b, q, start + r * 16, 16), pl.ds(pl.multiple_of(start + r * 16, 16), 16))

    def add_in(b, d, mq, q, h):
        start, size, cs = part_of(b, d, mq, h)

        def body(rr, _):
            ring[d, rr, cs] = ring[d, rr, cs] + part[rr, cs]
        row_loop(b, q, start, size, body)

    def group1(b):
        if b == 0:
            turns = ((3, 0), (0, 0), (3, 1), (2, 0), (0, 1))
        else:
            turns = ((3, 0), (3, 1), (0, 0), (2, 0), (0, 1), (2, 1))

        @pl.when(inner == 1)
        def _():
            for mq, h in turns:
                if mq:
                    wait_near(b, mq, h)
                    add_in(b, side, mq, mirror(mq), h)
                    near_copy(ring.at[side], b, mq, h, far_index(b, 3 - mq, h)).start()
                else:
                    wait_far(b, 0, h)
                    add_in(b, 1 - side, 3, mirror(0), h)
                    far_copy(b, 0, h).start()

    def hand_over():
        return pltpu.make_async_remote_copy(
            out.at[2], got, t_send, t_recv, device_id={"g": (g + 1) % NG}, device_id_type=MESH)

    def group2(b):
        slot = (0, 1 + last, (5 - g) // 2)[b]

        @pl.when(inner == 1)
        def _():
            q = mirror(1)
            for h in range(pieces(b, 1)):
                wait_far(b, 1, h)
                wait_near(b, 1, h)
                if b:
                    def body(rr, ro):
                        out[slot, ro] = ring[0, rr] + part[rr] + ring[1, rr]
                    row_loop(b, q, h * HALF, HALF, body)

        if b == 0:
            one, mid = SENT[2], SENT[1]
            lo = ROWS - one

            @pl.when(z == 1)
            def _():
                q1 = pl.ds(QR, QR)
                turned = ring[1, 0:lo, lo:mid].T
                out[0, :, 0:lo] = ring[0, q1, 0:lo] + turned[mid - lo - QR:]
                out[0, :, lo:mid] = ring[0, q1, lo:mid] + part[q1, lo:mid] + ring[1, q1, lo:mid]
                turned = ring[0, 2 * QR:ROWS, lo:mid].T
                out[0, :, mid:] = ring[1, q1, mid:] + turned[mid - lo - QR:]

            @pl.when(z == 2)
            def _():
                q2 = pl.ds(2 * QR, QR)
                turned = ring[0, one:ROWS, mid:one].T
                out[0, :, one:] = ring[1, q2, one:] + turned[:QR]
                out[0, :, mid:one] = ring[0, q2, mid:one] + part[q2, mid:one] + ring[1, q2, mid:one]
                turned = ring[1, 0:2 * QR, mid:one].T
                out[0, :, :mid] = ring[0, q2, :mid] + turned[:QR]

        @pl.when(inner == 0)
        def _():
            q = mirror(0)
            for h in range(pieces(b, 3)):
                wait_far(b, 0, h)
                start, size, cs = part_of(b, 1 - side, 3, h)

                def body(rr, ro):
                    out[slot, ro, cs] = ring[1 - side, rr, cs] + part[rr, cs]
                row_loop(b, q, start, size, body)

        if b == 1:
            @pl.when(last == 1)
            def _():
                hand_over().start()

    def fill(value):
        @pl.loop(0, QR // 16)
        def _(r):
            rs = pl.ds(pl.multiple_of(r * 16, 16), 16)
            out[2, rs] = value(rs)

    start()
    compute(0)
    group1(0)
    compute(1)
    group2(0)
    group1(1)

    @pl.when(has3 == 1)
    def _():
        compute(2)

    group2(1)

    @pl.when(has3 == 1)
    def _():
        group1(2)
        group2(2)

    @pl.when(g == 0)
    def _():
        hand_over().wait_recv()
        fill(lambda rs: got[rs])

    def drain_rows(ref):
        return pltpu.make_async_remote_copy(ref, ref, a_send, a_recv.at[0, 0],
                                            device_id={"g": (g + 1) % NG}, device_id_type=MESH)

    @pl.when(g == 2)
    def _():
        drain_rows(abuf).wait_send()

    @pl.when(g != 2)
    def _():
        drain_rows(abuf.at[0]).wait_send()

    @pl.when(last == 1)
    def _():
        hand_over().wait_send()

    @pl.when(g >= 2)
    def _():
        fill(lambda rs: jnp.zeros((16, ROWS), jnp.float32))

    first = (sum(SENT.values()) * QR // ROWS, (2 * SENT[3] + SENT[2]) * QR // ROWS)
    for i in range(2):
        for k in range(2):
            @pl.when((inner == i) & (has3 == k))
            def _():
                ref = part.at[pl.ds(0, first[i] + (1 + k) * 3 * QR)]
                pltpu.make_async_remote_copy(ref, ref, z_send, z_recv.at[0],
                                             device_id={"kk": toward}, device_id_type=MESH).wait_send()


def solution(mesh):
    def local_fn(a_blk):
        cols = a_blk.shape[1]
        dma = pltpu.SemaphoreType.DMA
        out = pl.pallas_call(
            kernel,
            out_shape=jax.ShapeDtypeStruct((3, QR, ROWS), jnp.float32),
            in_specs=[pl.BlockSpec(memory_space=pltpu.HBM)],
            out_specs=pl.BlockSpec(memory_space=pltpu.VMEM),
            scratch_shapes=[
                pltpu.VMEM((3, ROWS, cols), jnp.bfloat16),
                pltpu.VMEM((3 * ROWS, ROWS), jnp.float32),
                pltpu.VMEM((2, 3 * ROWS, ROWS), jnp.float32),
                pltpu.VMEM((QR, ROWS), jnp.float32),
                dma((2,)), dma, dma((2, NZ)), dma, dma((NRECV,)), dma, dma,
            ],
            compiler_params=pltpu.CompilerParams(
                collective_id=0, has_side_effects=True, vmem_limit_bytes=50 * 2**20),
        )(a_blk)
        return out[None]

    return jax.shard_map(local_fn, mesh=mesh, in_specs=(P(("m", "g"), "kk"),),
                         out_specs=P(("m", "g"), None, "kk", None), check_vma=False)
```

```python
import jax
import jax.numpy as jnp
from jax import lax
from jax.experimental import pallas as pl
from jax.experimental.pallas import tpu as pltpu
from jax.sharding import PartitionSpec as P

MESH = pl.DeviceIdType.MESH
NZ = 4
NG = 4
ROWS = 768
QR = ROWS // NZ
HALF = QR // 2
FIRST = 128
ONE, MID = 640, 384
SENT = {
    3: ((0, QR, ONE, FIRST), (64, QR - 64, 0, ONE), (0, 64, 0, MID), (0, 64, 512, FIRST)),
    2: ((0, QR, 0, ONE),),
    1: ((0, QR, 0, MID),),
}
EXTRA = (0, 64, MID, FIRST)


def pieces(b, mq):
    return 2 if b else len(SENT[mq])


def near_index(b, mq, h):
    base = 0
    for k in range(b):
        base += sum(pieces(k, m) for m in (3, 2, 1)) + pieces(k, 3) + pieces(k, 2)
    return base + sum(pieces(b, m) for m in (3, 2, 1) if m > mq) + h


def far_index(b, mq, h):
    return near_index(b, 0, 0) + (pieces(b, 3) if mq else 0) + h


NEXTRA = near_index(3, 3, 0)
NRECV = NEXTRA + 1


def elements(parts):
    return sum(p[1] * p[3] for p in parts)


def kernel(a_hbm, out, abuf, part, ring, got, load_sem, a_send, a_recv, z_send, z_recv, t_send, t_recv):
    z = lax.axis_index("kk")
    g = lax.axis_index("g")
    side = z // 2
    inner = ((z + 1) // 2) % 2
    has3 = g % 2
    last = g // 3
    toward = z + 1 - 2 * side
    away = z - 1 + 2 * side

    def mirror(q):
        return q + side * (3 - 2 * q)

    def order(i):
        return mirror(3 - i + inner * (i // 2) * (2 * i - 5))

    def load(k):
        size = (QR, ROWS - QR)[k]
        start = ((1 - side) * (ROWS - QR), side * QR)[k]
        rs = pl.ds(pl.multiple_of(start, QR), size)
        return pltpu.make_async_copy(a_hbm.at[rs], abuf.at[0, rs], load_sem.at[k])

    load(0).start()
    load(1).start()

    bar = pltpu.get_barrier_semaphore()
    for d in (1, NG - 1):
        pl.semaphore_signal(bar, inc=1, device_id={"g": (g + d) % NG}, device_id_type=MESH)
    pl.semaphore_signal(bar, inc=1, device_id={"kk": toward}, device_id_type=MESH)

    @pl.when(inner == 1)
    def _():
        pl.semaphore_signal(bar, inc=1, device_id={"kk": away}, device_id_type=MESH)

    def chunk(q):
        return pl.ds(pl.multiple_of(q * QR, QR), QR)

    def row_copy(src, slot, q, d):
        return pltpu.make_async_remote_copy(
            src.at[chunk(q)], abuf.at[slot, chunk(q)], a_send, a_recv.at[slot - 1, q],
            device_id={"g": (g + d) % NG}, device_id_type=MESH)

    def arrival(slot, q):
        return row_copy(a_hbm, slot, q, NG - 1)

    def dot(x, y):
        return lax.dot_general(x, y, (((1,), (1,)), ((), ())), preferred_element_type=jnp.float32)

    def at(b, q, start, size):
        return pl.ds(pl.multiple_of(b * ROWS + q * QR + start, 16), size)

    def product(b, q):
        left = (0, 1 + last, 2 - last)[b]
        right = (0, last, 0)[b]
        part[at(b, q, 0, QR)] = dot(abuf[left, chunk(q)], abuf[right])

    def part_of(b, d, piece):
        if b:
            return piece * HALF, HALF, pl.ds(0, ROWS)
        row, nrows, col, ncols = piece
        row = row + d * (QR - 2 * row - nrows)
        col = col + d * (ROWS - 2 * col - ncols)
        return row, nrows, pl.ds(pl.multiple_of(col, 128), ncols)

    def piece_of(b, mq, h):
        return h if b else SENT[mq][h]

    def z_copy(src, b, d, piece, q, dev, index):
        start, size, cs = part_of(b, d, piece)
        return pltpu.make_async_remote_copy(
            src.at[at(b, q, start, size), cs], ring.at[d, at(b, q, start, size), cs],
            z_send, z_recv.at[index], device_id={"kk": dev}, device_id_type=MESH)

    def near_copy(src, b, mq, h, index):
        return z_copy(src, b, side, piece_of(b, mq, h), mirror(mq), toward, index)

    def far_copy(b, mq, h):
        d = 1 - side
        return z_copy(ring.at[d], b, d, piece_of(b, 3 - mq, h), mirror(mq), away, far_index(b, mq, h))

    def extra_copy():
        d = 1 - side
        return z_copy(ring.at[d], 0, d, EXTRA, mirror(0), away, NEXTRA)

    def wait_near(b, mq, h):
        near_copy(part, b, mq, h, near_index(b, mq, h)).wait_recv()

    def wait_far(b, mq, h):
        far_copy(b, mq, h).wait_recv()

    def send_near(b, mq):
        for h in range(pieces(b, mq)):
            near_copy(part, b, mq, h, near_index(b, mq, h)).start()

    def start():
        q = order(0)
        cs = pl.ds(pl.multiple_of((1 - side) * (ROWS - FIRST), FIRST), FIRST)
        load(0).wait()
        part[at(0, q, 0, QR), cs] = dot(abuf[0, chunk(q)], abuf[0, cs])
        pl.semaphore_wait(bar, 3 + inner)

        @pl.when(inner == 0)
        def _():
            near_copy(part, 0, 3, 0, near_index(0, 3, 0)).start()

        @pl.loop(0, NZ)
        def _(i):
            row_copy(a_hbm, 1, order(i), NG - 1).start()

        @pl.when(g == 2)
        def _():
            @pl.loop(0, NZ)
            def _(i):
                row_copy(a_hbm, 2, order(i), 1).start()

        cs = pl.ds(pl.multiple_of(side * FIRST, FIRST), ROWS - FIRST)
        load(1).wait()
        part[at(0, q, 0, QR), cs] = dot(abuf[0, chunk(q)], abuf[0, cs])

        @pl.when(inner == 0)
        def _():
            for h in range(1, pieces(0, 3)):
                near_copy(part, 0, 3, h, near_index(0, 3, h)).start()

    def compute(b):
        def step(i):
            q = order(i)
            if b == 1:
                @pl.when(last == 0)
                def _():
                    arrival(1, q).wait_recv()

                @pl.when(g == 2)
                def _():
                    row_copy(abuf.at[1], 2, q, NG - 1).start()

                @pl.when(last == 1)
                def _():
                    arrival(2, q).wait_recv()
            if b == 2:
                @pl.when(g == 1)
                def _():
                    arrival(2, q).wait_recv()
            product(b, q)
            for k in range(0 if b else 1, 3):
                @pl.when((inner == 0) & (i == k))
                def _():
                    send_near(b, 3 - k)

        if b == 1:
            @pl.when(last == 1)
            def _():
                for q in range(NZ):
                    arrival(1, q).wait_recv()
        pl.loop(0 if b else 1, NZ)(step)

    def row_loop(b, q, start, size, body):
        @pl.loop(0, size // 16)
        def _(r):
            body(at(b, q, start + r * 16, 16), pl.ds(pl.multiple_of(start + r * 16, 16), 16))

    def add_in(b, d, mq, q, h):
        start, size, cs = part_of(b, d, piece_of(b, mq, h))

        def body(rr, _):
            ring[d, rr, cs] = ring[d, rr, cs] + part[rr, cs]
        row_loop(b, q, start, size, body)

    def group1(b):
        if b == 0:
            turns = ((3, 0), (0, 0), (3, 1), (3, 2), (3, 3), (2, 0), (0, 1), (0, 2), (0, 3))
        else:
            turns = ((3, 0), (3, 1), (0, 0), (2, 0), (0, 1), (2, 1))

        @pl.when(inner == 1)
        def _():
            for mq, h in turns:
                if mq:
                    wait_near(b, mq, h)
                    add_in(b, side, mq, mirror(mq), h)
                    near_copy(ring.at[side], b, mq, h, far_index(b, 3 - mq, h)).start()
                else:
                    wait_far(b, 0, h)
                    add_in(b, 1 - side, 3, mirror(0), h)
                    far_copy(b, 0, h).start()

    def hand_over():
        return pltpu.make_async_remote_copy(
            out.at[2], got, t_send, t_recv, device_id={"g": (g + 1) % NG}, device_id_type=MESH)

    def fill_in():
        @pl.when(z == 1)
        def _():
            turned = ring[1, 256:384, 128:256].T
            ring[1, 128:192, 256:384] = turned[:64] + part[128:192, 256:384]

        @pl.when(z == 2)
        def _():
            turned = ring[0, 384:512, 512:640].T
            ring[0, 576:640, 384:512] = turned[64:] + part[576:640, 384:512]

    def group2(b):
        slot = (0, 1 + last, (5 - g) // 2)[b]

        @pl.when(inner == 1)
        def _():
            q = mirror(1)
            for h in range(pieces(b, 1)):
                wait_far(b, 1, h)
                if b == 0:
                    fill_in()
                    extra_copy().start()
                wait_near(b, 1, h)
                if b:
                    def body(rr, ro):
                        out[slot, ro] = ring[0, rr] + part[rr] + ring[1, rr]
                    row_loop(b, q, h * HALF, HALF, body)

        if b == 0:
            lo = ROWS - ONE

            @pl.when(z == 1)
            def _():
                q1 = pl.ds(QR, QR)
                turned = ring[1, 0:lo, lo:MID].T
                out[0, :, 0:lo] = ring[0, q1, 0:lo] + turned[MID - lo - QR:]
                out[0, :, lo:MID] = ring[0, q1, lo:MID] + part[q1, lo:MID] + ring[1, q1, lo:MID]
                turned = ring[0, 2 * QR:ROWS, lo:MID].T
                out[0, :, MID:] = ring[1, q1, MID:] + turned[MID - lo - QR:]

            @pl.when(z == 2)
            def _():
                q2 = pl.ds(2 * QR, QR)
                turned = ring[0, ONE:ROWS, MID:ONE].T
                out[0, :, ONE:] = ring[1, q2, ONE:] + turned[:QR]
                out[0, :, MID:ONE] = ring[0, q2, MID:ONE] + part[q2, MID:ONE] + ring[1, q2, MID:ONE]
                turned = ring[1, 0:2 * QR, MID:ONE].T
                out[0, :, :MID] = ring[0, q2, :MID] + turned[:QR]

        @pl.when(inner == 0)
        def _():
            q = mirror(0)

            def add_out(piece):
                start, size, cs = part_of(b, 1 - side, piece)

                def body(rr, ro):
                    out[slot, ro, cs] = ring[1 - side, rr, cs] + part[rr, cs]
                row_loop(b, q, start, size, body)

            for h in range(pieces(b, 3)):
                wait_far(b, 0, h)
                add_out(piece_of(b, 3, h))
            if b == 0:
                extra_copy().wait_recv()
                add_out(EXTRA)

        if b == 1:
            @pl.when(last == 1)
            def _():
                hand_over().start()

    def fill(value):
        @pl.loop(0, QR // 16)
        def _(r):
            rs = pl.ds(pl.multiple_of(r * 16, 16), 16)
            out[2, rs] = value(rs)

    start()
    compute(0)
    group1(0)
    compute(1)
    group2(0)
    group1(1)

    @pl.when(has3 == 1)
    def _():
        compute(2)

    group2(1)

    @pl.when(has3 == 1)
    def _():
        group1(2)
        group2(2)

    @pl.when(g == 0)
    def _():
        hand_over().wait_recv()
        fill(lambda rs: got[rs])

    def drain_rows(ref):
        return pltpu.make_async_remote_copy(ref, ref, a_send, a_recv.at[0, 0],
                                            device_id={"g": (g + 1) % NG}, device_id_type=MESH)

    @pl.when(g == 2)
    def _():
        drain_rows(abuf).wait_send()

    @pl.when(g != 2)
    def _():
        drain_rows(abuf.at[0]).wait_send()

    @pl.when(last == 1)
    def _():
        hand_over().wait_send()

    @pl.when(g >= 2)
    def _():
        fill(lambda rs: jnp.zeros((16, ROWS), jnp.float32))

    first = (elements(SENT[3] + SENT[2] + SENT[1]), elements(2 * SENT[3] + SENT[2] + (EXTRA,)))
    for i in range(2):
        for k in range(2):
            @pl.when((inner == i) & (has3 == k))
            def _():
                total = first[i] + (1 + k) * 3 * QR * ROWS
                ref = ring.at[:, pl.ds(0, total // 1024), pl.ds(0, 512)]
                pltpu.make_async_remote_copy(ref, ref, z_send, z_recv.at[0],
                                             device_id={"kk": toward}, device_id_type=MESH).wait_send()


def solution(mesh):
    def local_fn(a_blk):
        cols = a_blk.shape[1]
        dma = pltpu.SemaphoreType.DMA
        out = pl.pallas_call(
            kernel,
            out_shape=jax.ShapeDtypeStruct((3, QR, ROWS), jnp.float32),
            in_specs=[pl.BlockSpec(memory_space=pltpu.HBM)],
            out_specs=pl.BlockSpec(memory_space=pltpu.VMEM),
            scratch_shapes=[
                pltpu.VMEM((3, ROWS, cols), jnp.bfloat16),
                pltpu.VMEM((3 * ROWS, ROWS), jnp.float32),
                pltpu.VMEM((2, 3 * ROWS, ROWS), jnp.float32),
                pltpu.VMEM((QR, ROWS), jnp.float32),
                dma((2,)), dma, dma((2, NZ)), dma, dma((NRECV,)), dma, dma,
            ],
            compiler_params=pltpu.CompilerParams(
                collective_id=0, has_side_effects=True, vmem_limit_bytes=50 * 2**20),
        )(a_blk)
        return out[None]

    return jax.shard_map(local_fn, mesh=mesh, in_specs=(P(("m", "g"), "kk"),),
                         out_specs=P(("m", "g"), None, "kk", None), check_vma=False)
```

```python
import jax
import jax.numpy as jnp
from jax import lax
from jax.experimental import pallas as pl
from jax.experimental.pallas import tpu as pltpu
from jax.sharding import PartitionSpec as P

MESH = pl.DeviceIdType.MESH
NZ = 4
NG = 4
ROWS = 768
QR = ROWS // NZ
HALF = QR // 2
FIRST = 128
TILE = 128
SENT = {
    3: ((64, TILE, ROWS - FIRST, FIRST), (0, QR, 0, ROWS - FIRST)),
    2: ((0, QR, 0, 512), (128, 64, 512, TILE)),
    1: ((0, QR, 0, 256), (64, 128, 256, TILE)),
}


def pieces(b, mq):
    return 2 if b else len(SENT[mq])


def near_index(b, mq, h):
    base = 0
    for k in range(b):
        base += sum(pieces(k, m) for m in (3, 2, 1)) + pieces(k, 3) + pieces(k, 2)
    return base + sum(pieces(b, m) for m in (3, 2, 1) if m > mq) + h


def far_index(b, mq, h):
    return near_index(b, 0, 0) + (pieces(b, 3) if mq else 0) + h


NRECV = near_index(3, 3, 0)


def elements(parts):
    return sum(p[1] * p[3] for p in parts)


def kernel(a_hbm, out, abuf, part, ring, got, load_sem, a_send, a_recv, z_send, z_recv, t_send, t_recv):
    z = lax.axis_index("kk")
    g = lax.axis_index("g")
    side = z // 2
    inner = ((z + 1) // 2) % 2
    has3 = g % 2
    last = g // 3
    toward = z + 1 - 2 * side
    away = z - 1 + 2 * side

    def mirror(q):
        return q + side * (3 - 2 * q)

    def order(i):
        return mirror(3 - i + inner * (i // 2) * (2 * i - 5))

    def load(k):
        size = (QR, ROWS - QR)[k]
        start = ((1 - side) * (ROWS - QR), side * QR)[k]
        rs = pl.ds(pl.multiple_of(start, QR), size)
        return pltpu.make_async_copy(a_hbm.at[rs], abuf.at[0, rs], load_sem.at[k])

    load(0).start()
    load(1).start()

    bar = pltpu.get_barrier_semaphore()
    for d in (1, NG - 1):
        pl.semaphore_signal(bar, inc=1, device_id={"g": (g + d) % NG}, device_id_type=MESH)
    pl.semaphore_signal(bar, inc=1, device_id={"kk": toward}, device_id_type=MESH)

    @pl.when(inner == 1)
    def _():
        pl.semaphore_signal(bar, inc=1, device_id={"kk": away}, device_id_type=MESH)

    def chunk(q):
        return pl.ds(pl.multiple_of(q * QR, QR), QR)

    def row_copy(src, slot, q, d):
        return pltpu.make_async_remote_copy(
            src.at[chunk(q)], abuf.at[slot, chunk(q)], a_send, a_recv.at[slot - 1, q],
            device_id={"g": (g + d) % NG}, device_id_type=MESH)

    def arrival(slot, q):
        return row_copy(a_hbm, slot, q, NG - 1)

    def dot(x, y):
        return lax.dot_general(x, y, (((1,), (1,)), ((), ())), preferred_element_type=jnp.float32)

    def at(b, q, start, size):
        return pl.ds(pl.multiple_of(b * ROWS + q * QR + start, 16), size)

    def product(b, q):
        left = (0, 1 + last, 2 - last)[b]
        right = (0, last, 0)[b]
        part[at(b, q, 0, QR)] = dot(abuf[left, chunk(q)], abuf[right])

    def part_of(b, d, piece):
        if b:
            return piece * HALF, HALF, pl.ds(0, ROWS)
        row, nrows, col, ncols = piece
        row = row + d * (QR - 2 * row - nrows)
        col = col + d * (ROWS - 2 * col - ncols)
        return row, nrows, pl.ds(pl.multiple_of(col, 128), ncols)

    def piece_of(b, mq, h):
        return h if b else SENT[mq][h]

    def z_copy(src, b, d, piece, q, dev, index):
        start, size, cs = part_of(b, d, piece)
        return pltpu.make_async_remote_copy(
            src.at[at(b, q, start, size), cs], ring.at[d, at(b, q, start, size), cs],
            z_send, z_recv.at[index], device_id={"kk": dev}, device_id_type=MESH)

    def near_copy(src, b, mq, h, index):
        return z_copy(src, b, side, piece_of(b, mq, h), mirror(mq), toward, index)

    def far_copy(b, mq, h):
        d = 1 - side
        return z_copy(ring.at[d], b, d, piece_of(b, 3 - mq, h), mirror(mq), away, far_index(b, mq, h))

    def wait_near(b, mq, h):
        near_copy(part, b, mq, h, near_index(b, mq, h)).wait_recv()

    def wait_far(b, mq, h):
        far_copy(b, mq, h).wait_recv()

    def send_near(b, mq):
        for h in range(pieces(b, mq)):
            near_copy(part, b, mq, h, near_index(b, mq, h)).start()

    def start():
        q = order(0)
        cs = pl.ds(pl.multiple_of((1 - side) * (ROWS - FIRST), FIRST), FIRST)
        load(0).wait()
        part[at(0, q, 0, QR), cs] = dot(abuf[0, chunk(q)], abuf[0, cs])
        pl.semaphore_wait(bar, 3 + inner)

        @pl.when(inner == 0)
        def _():
            near_copy(part, 0, 3, 0, near_index(0, 3, 0)).start()

        @pl.loop(0, NZ)
        def _(i):
            row_copy(a_hbm, 1, order(i), NG - 1).start()

        @pl.when(g == 2)
        def _():
            @pl.loop(0, NZ)
            def _(i):
                row_copy(a_hbm, 2, order(i), 1).start()

        cs = pl.ds(pl.multiple_of(side * FIRST, FIRST), ROWS - FIRST)
        load(1).wait()
        part[at(0, q, 0, QR), cs] = dot(abuf[0, chunk(q)], abuf[0, cs])

        @pl.when(inner == 0)
        def _():
            for h in range(1, pieces(0, 3)):
                near_copy(part, 0, 3, h, near_index(0, 3, h)).start()

    def compute(b, first, stop):
        def step(i):
            q = order(i)
            if b == 1:
                @pl.when(g < 2)
                def _():
                    arrival(1, q).wait_recv()

                @pl.when(last == 1)
                def _():
                    arrival(2, q).wait_recv()
            if b == 2:
                @pl.when(g == 1)
                def _():
                    arrival(2, q).wait_recv()
            product(b, q)
            for k in range(first, min(stop, 3)):
                @pl.when((inner == 0) & (i == k))
                def _():
                    send_near(b, 3 - k)

        if b == 1 and first == 0:
            @pl.when(last == 1)
            def _():
                for q in range(NZ):
                    arrival(1, q).wait_recv()
        pl.loop(first, stop)(step)

    def row_loop(b, q, start, size, body):
        @pl.loop(0, size // 16)
        def _(r):
            body(at(b, q, start + r * 16, 16), pl.ds(pl.multiple_of(start + r * 16, 16), 16))

    def add_in(b, d, mq, q, h):
        start, size, cs = part_of(b, d, piece_of(b, mq, h))

        def body(rr, _):
            ring[d, rr, cs] = ring[d, rr, cs] + part[rr, cs]
        row_loop(b, q, start, size, body)

    def group1(b):
        if b == 0:
            turns = ((3, 0), (0, 0), (3, 1), (2, 0), (2, 1), (0, 1))
        else:
            turns = ((3, 0), (3, 1), (0, 0), (2, 0), (0, 1), (2, 1))

        @pl.when(inner == 1)
        def _():
            for mq, h in turns:
                if mq:
                    wait_near(b, mq, h)
                    add_in(b, side, mq, mirror(mq), h)
                    near_copy(ring.at[side], b, mq, h, far_index(b, 3 - mq, h)).start()
                else:
                    wait_far(b, 0, h)
                    add_in(b, 1 - side, 3, mirror(0), h)
                    far_copy(b, 0, h).start()

    def hand_over():
        return pltpu.make_async_remote_copy(
            out.at[2], got, t_send, t_recv, device_id={"g": (g + 1) % NG}, device_id_type=MESH)

    def finish_inner(q, near, far, turn):
        low = turn == 0

        def cols(start, size):
            return pl.ds(start if low else ROWS - start - size, size)

        def rows_of(start, size):
            return cols(start, size)

        def turned(d, row, nrows, narrow):
            x = ring[d, rows_of(row, nrows), cols(128 if narrow else 256, TILE)].T
            if narrow:
                x = x[64:] if low else x[:64]
            return x

        def put(row, nrows, col, ncols, value):
            start = (row if low else ROWS - row - nrows) - q * QR
            out[0, start:start + nrows, cols(col, ncols)] = value

        def get(ref, row, nrows, col, ncols):
            return ref[rows_of(row, nrows), cols(col, ncols)]

        n, f = ring.at[near], ring.at[far]
        a, b = (192, 64), (256, 128)
        put(*a, 0, 128, get(n, *a, 0, 128) + turned(far, 0, 128, True))
        put(*a, 128, 128, get(n, *a, 128, 128) + get(part, *a, 128, 128) + get(f, *a, 128, 128))
        put(*a, 256, 128, turned(near, 256, 128, True) + get(part, *a, 256, 128) + get(f, *a, 256, 128))
        put(*a, 384, 384, turned(near, 384, 384, True) + get(f, *a, 384, 384))
        lane = lax.broadcasted_iota(jnp.int32, (128, 256), 1)
        mine = jnp.where(lane >= 192 if low else lane < 64, get(part, *b, 0, 256), 0.0)
        put(*b, 0, 256, get(n, *b, 0, 256) + turned(far, 0, 256, False) + mine)
        put(*b, 256, 128, get(n, *b, 256, 128) + get(part, *b, 256, 128) + get(f, *b, 256, 128))
        put(*b, 384, 384, turned(near, 384, 384, False) + get(f, *b, 384, 384))

    def group2(b):
        slot = (0, 1 + last, (5 - g) // 2)[b]

        @pl.when(inner == 1)
        def _():
            q = mirror(1)
            for h in range(pieces(b, 1)):
                wait_far(b, 1, h)
                wait_near(b, 1, h)
                if b:
                    def body(rr, ro):
                        out[slot, ro] = ring[0, rr] + part[rr] + ring[1, rr]
                    row_loop(b, q, h * HALF, HALF, body)

        if b == 0:
            @pl.when(z == 1)
            def _():
                finish_inner(1, 0, 1, 0)

            @pl.when(z == 2)
            def _():
                finish_inner(2, 1, 0, 1)

        @pl.when(inner == 0)
        def _():
            q = mirror(0)

            def add_out(piece):
                start, size, cs = part_of(b, 1 - side, piece)

                def body(rr, ro):
                    out[slot, ro, cs] = ring[1 - side, rr, cs] + part[rr, cs]
                row_loop(b, q, start, size, body)

            for h in range(pieces(b, 3)):
                wait_far(b, 0, h)
                add_out(piece_of(b, 3, h))

        if b == 0:
            @pl.when(z == 0)
            def _():
                turned = ring[1, 0:128, 128:256].T
                out[0, 128:192, 0:128] = part[128:192, 0:128] + turned[:64]

            @pl.when(z == 3)
            def _():
                turned = ring[0, 640:768, 512:640].T
                out[0, 0:64, 640:768] = part[576:640, 640:768] + turned[64:]

        if b == 1:
            @pl.when(last == 1)
            def _():
                hand_over().start()

    def fill(value):
        @pl.loop(0, QR // 16)
        def _(r):
            rs = pl.ds(pl.multiple_of(r * 16, 16), 16)
            out[2, rs] = value(rs)

    start()
    compute(0, 1, NZ)

    @pl.when(g == 2)
    def _():
        @pl.loop(0, NZ)
        def _(i):
            q = order(i)
            arrival(1, q).wait_recv()
            row_copy(abuf.at[1], 2, q, NG - 1).start()

    group1(0)
    compute(1, 0, 3)
    group2(0)
    group1(1)
    compute(1, 3, NZ)

    @pl.when(has3 == 1)
    def _():
        compute(2, 0, 3)

    group2(1)

    @pl.when(has3 == 1)
    def _():
        group1(2)
        compute(2, 3, NZ)
        group2(2)

    @pl.when(g == 0)
    def _():
        hand_over().wait_recv()
        fill(lambda rs: got[rs])

    def drain_rows(ref):
        return pltpu.make_async_remote_copy(ref, ref, a_send, a_recv.at[0, 0],
                                            device_id={"g": (g + 1) % NG}, device_id_type=MESH)

    @pl.when(g == 2)
    def _():
        drain_rows(abuf).wait_send()

    @pl.when(g != 2)
    def _():
        drain_rows(abuf.at[0]).wait_send()

    @pl.when(last == 1)
    def _():
        hand_over().wait_send()

    @pl.when(g >= 2)
    def _():
        fill(lambda rs: jnp.zeros((16, ROWS), jnp.float32))

    first = (elements(SENT[3] + SENT[2] + SENT[1]), elements(2 * SENT[3] + SENT[2]))
    for i in range(2):
        for k in range(2):
            @pl.when((inner == i) & (has3 == k))
            def _():
                total = first[i] + (1 + k) * 3 * QR * ROWS
                ref = ring.at[:, pl.ds(0, total // 1024), pl.ds(0, 512)]
                pltpu.make_async_remote_copy(ref, ref, z_send, z_recv.at[0],
                                             device_id={"kk": toward}, device_id_type=MESH).wait_send()


def solution(mesh):
    def local_fn(a_blk):
        cols = a_blk.shape[1]
        dma = pltpu.SemaphoreType.DMA
        out = pl.pallas_call(
            kernel,
            out_shape=jax.ShapeDtypeStruct((3, QR, ROWS), jnp.float32),
            in_specs=[pl.BlockSpec(memory_space=pltpu.HBM)],
            out_specs=pl.BlockSpec(memory_space=pltpu.VMEM),
            scratch_shapes=[
                pltpu.VMEM((3, ROWS, cols), jnp.bfloat16),
                pltpu.VMEM((3 * ROWS, ROWS), jnp.float32),
                pltpu.VMEM((2, 3 * ROWS, ROWS), jnp.float32),
                pltpu.VMEM((QR, ROWS), jnp.float32),
                dma((2,)), dma, dma((2, NZ)), dma, dma((NRECV,)), dma, dma,
            ],
            compiler_params=pltpu.CompilerParams(
                collective_id=0, has_side_effects=True, vmem_limit_bytes=50 * 2**20),
        )(a_blk)
        return out[None]

    return jax.shard_map(local_fn, mesh=mesh, in_specs=(P(("m", "g"), "kk"),),
                         out_specs=P(("m", "g"), None, "kk", None), check_vma=False)
```

```python
import jax
import jax.numpy as jnp
from jax import lax
from jax.experimental import pallas as pl
from jax.experimental.pallas import tpu as pltpu
from jax.sharding import PartitionSpec as P

MESH = pl.DeviceIdType.MESH
NZ = 4
NG = 4
ROWS = 768
QR = ROWS // NZ
HALF = QR // 2
FIRST = 256
TILE = 128
SENT = {
    3: ((0, QR, 512, TILE), (128, 64, 640, TILE), (0, QR, 0, 512)),
    2: ((0, QR, 0, 384), (64, 128, 384, TILE)),
    1: ((0, QR, 0, 256), (128, 64, 256, TILE)),
}
PACKED = ((384, 512), (256, 640))


def pieces(b, mq):
    return 2 if b else len(SENT[mq])


def near_index(b, mq, h):
    base = 0
    for k in range(b):
        base += sum(pieces(k, m) for m in (3, 2, 1)) + pieces(k, 3) + pieces(k, 2)
    return base + sum(pieces(b, m) for m in (3, 2, 1) if m > mq) + h


def far_index(b, mq, h):
    return near_index(b, 0, 0) + (pieces(b, 3) if mq else 0) + h


NRECV = near_index(3, 3, 0)


def elements(parts):
    return sum(p[1] * p[3] for p in parts)


def kernel(a_hbm, out, abuf, part, ring, got, pack_in, pack_out, load_sem, a_send, a_recv, z_send, z_recv,
           p_recv, t_send, t_recv):
    z = lax.axis_index("kk")
    g = lax.axis_index("g")
    side = z // 2
    inner = ((z + 1) // 2) % 2
    has3 = g % 2
    last = g // 3
    toward = z + 1 - 2 * side
    away = z - 1 + 2 * side

    def mirror(q):
        return q + side * (3 - 2 * q)

    def order(i):
        return mirror(3 - i + inner * (i // 2) * (2 * i - 5))

    def load(k):
        size = (FIRST, ROWS - FIRST)[k]
        start = ((1 - side) * (ROWS - FIRST), side * FIRST)[k]
        rs = pl.ds(pl.multiple_of(start, FIRST), size)
        return pltpu.make_async_copy(a_hbm.at[rs], abuf.at[0, rs], load_sem.at[k])

    load(0).start()
    load(1).start()

    bar = pltpu.get_barrier_semaphore()
    for d in (1, NG - 1):
        pl.semaphore_signal(bar, inc=1, device_id={"g": (g + d) % NG}, device_id_type=MESH)
    pl.semaphore_signal(bar, inc=1, device_id={"kk": toward}, device_id_type=MESH)

    @pl.when(inner == 1)
    def _():
        pl.semaphore_signal(bar, inc=1, device_id={"kk": away}, device_id_type=MESH)

    def chunk(q):
        return pl.ds(pl.multiple_of(q * QR, QR), QR)

    def row_copy(src, slot, q, d):
        return pltpu.make_async_remote_copy(
            src.at[chunk(q)], abuf.at[slot, chunk(q)], a_send, a_recv.at[slot - 1, q],
            device_id={"g": (g + d) % NG}, device_id_type=MESH)

    def arrival(slot, q):
        return row_copy(a_hbm, slot, q, NG - 1)

    def dot(x, y):
        return lax.dot_general(x, y, (((1,), (1,)), ((), ())), preferred_element_type=jnp.float32)

    def at(b, q, start, size):
        return pl.ds(pl.multiple_of(b * ROWS + q * QR + start, 16), size)

    def product(b, q):
        left = (0, 1 + last, 2 - last)[b]
        right = (0, last, 0)[b]
        part[at(b, q, 0, QR)] = dot(abuf[left, chunk(q)], abuf[right])

    def part_of(b, d, piece):
        if b:
            return piece * HALF, HALF, pl.ds(0, ROWS)
        row, nrows, col, ncols = piece
        row = row + d * (QR - 2 * row - nrows)
        col = col + d * (ROWS - 2 * col - ncols)
        return row, nrows, pl.ds(pl.multiple_of(col, 128), ncols)

    def piece_of(b, mq, h):
        return h if b else SENT[mq][h]

    def z_copy(src, b, d, piece, q, dev, index):
        start, size, cs = part_of(b, d, piece)
        return pltpu.make_async_remote_copy(
            src.at[at(b, q, start, size), cs], ring.at[d, at(b, q, start, size), cs],
            z_send, z_recv.at[index], device_id={"kk": dev}, device_id_type=MESH)

    def near_copy(src, b, mq, h, index):
        return z_copy(src, b, side, piece_of(b, mq, h), mirror(mq), toward, index)

    def far_copy(b, mq, h):
        d = 1 - side
        return z_copy(ring.at[d], b, d, piece_of(b, 3 - mq, h), mirror(mq), away, far_index(b, mq, h))

    def wait_near(b, mq, h):
        near_copy(part, b, mq, h, near_index(b, mq, h)).wait_recv()

    def wait_far(b, mq, h):
        far_copy(b, mq, h).wait_recv()

    def send_near(b, mq):
        for h in range(pieces(b, mq)):
            near_copy(part, b, mq, h, near_index(b, mq, h)).start()

    def start():
        q = order(0)
        cs = pl.ds(pl.multiple_of((1 - side) * (ROWS - FIRST), FIRST), FIRST)
        load(0).wait()
        part[at(0, q, 0, QR), cs] = dot(abuf[0, chunk(q)], abuf[0, cs])
        pl.semaphore_wait(bar, 3 + inner)

        @pl.when(inner == 0)
        def _():
            for h in range(2):
                near_copy(part, 0, 3, h, near_index(0, 3, h)).start()

        @pl.loop(0, NZ)
        def _(i):
            row_copy(a_hbm, 1, order(i), NG - 1).start()

        @pl.when(g == 2)
        def _():
            @pl.loop(0, NZ)
            def _(i):
                row_copy(a_hbm, 2, order(i), 1).start()

        cs = pl.ds(pl.multiple_of(side * FIRST, FIRST), ROWS - FIRST)
        load(1).wait()
        part[at(0, q, 0, QR), cs] = dot(abuf[0, chunk(q)], abuf[0, cs])

        @pl.when(inner == 0)
        def _():
            near_copy(part, 0, 3, 2, near_index(0, 3, 2)).start()

    def compute(b, first, stop):
        def step(i):
            q = order(i)
            if b == 1:
                @pl.when(g < 2)
                def _():
                    arrival(1, q).wait_recv()

                @pl.when(last == 1)
                def _():
                    arrival(2, q).wait_recv()
            if b == 2:
                @pl.when(g == 1)
                def _():
                    arrival(2, q).wait_recv()
            product(b, q)
            for k in range(first, min(stop, 3)):
                @pl.when((inner == 0) & (i == k))
                def _():
                    send_near(b, 3 - k)

        if b == 1 and first == 0:
            @pl.when(last == 1)
            def _():
                for q in range(NZ):
                    arrival(1, q).wait_recv()
        pl.loop(first, stop)(step)

    def row_loop(b, q, start, size, body):
        @pl.loop(0, size // 16)
        def _(r):
            body(at(b, q, start + r * 16, 16), pl.ds(pl.multiple_of(start + r * 16, 16), 16))

    def add_in(b, d, mq, q, h):
        start, size, cs = part_of(b, d, piece_of(b, mq, h))

        def body(rr, _):
            ring[d, rr, cs] = ring[d, rr, cs] + part[rr, cs]
        row_loop(b, q, start, size, body)

    def group1(b):
        if b == 0:
            turns = ((3, 0), (3, 1), (0, 0), (0, 1), (3, 2), (2, 0), (2, 1), (0, 2))
        else:
            turns = ((3, 0), (3, 1), (0, 0), (2, 0), (0, 1), (2, 1))

        @pl.when(inner == 1)
        def _():
            for mq, h in turns:
                if mq:
                    wait_near(b, mq, h)
                    add_in(b, side, mq, mirror(mq), h)
                    near_copy(ring.at[side], b, mq, h, far_index(b, 3 - mq, h)).start()
                else:
                    wait_far(b, 0, h)
                    add_in(b, 1 - side, 3, mirror(0), h)
                    far_copy(b, 0, h).start()

    def hand_over():
        return pltpu.make_async_remote_copy(
            out.at[2], got, t_send, t_recv, device_id={"g": (g + 1) % NG}, device_id_type=MESH)

    def flip(d, start, size):
        return pl.ds(ROWS - start - size if d else start, size)

    def get(ref, d, row, nrows, col, ncols):
        return ref[flip(d, row, nrows), flip(d, col, ncols)]

    def keep(d, x, y):
        lane = lax.broadcasted_iota(jnp.int32, x.shape, 1)
        return jnp.where(lane >= 64 if d else lane < 64, x, y)

    def roll(x):
        return pltpu.roll(x, 64, 1)

    def pack(d, slot):
        x, y = (get(part, d, row, 64, row, TILE) for row in PACKED[slot])
        return keep(d, x, roll(y))

    def unpack(d, slot, second):
        x = pack_in[d, pl.ds(slot * 64, 64)]
        return roll(x) if second else x

    def pack_copy(d, dev):
        return pltpu.make_async_remote_copy(
            pack_out.at[d], pack_in.at[d], z_send, p_recv.at[d], device_id={"kk": dev}, device_id_type=MESH)

    def pack_end(d):
        for slot in range(2):
            pack_out[d, pl.ds(slot * 64, 64)] = pack(d, slot)
        pack_copy(d, toward).start()

    def pack_pass(d, dev):
        pack_copy(d, dev).wait_recv()
        for slot in range(2):
            rs = pl.ds(slot * 64, 64)
            pack_out[d, rs] = pack_in[d, rs] + pack(d, slot)
        pack_copy(d, dev).start()

    def halves(d, x):
        return (x[64:], x[:64]) if d else (x[:64], x[64:])

    def finish_inner(q, near, far):
        d = near

        def put(row, nrows, col, ncols, value):
            start = (ROWS - row - nrows if d else row) - q * QR
            out[0, start:start + nrows, flip(d, col, ncols)] = value

        def turned(ref, row, nrows, col):
            return get(ref, d, row, nrows, col, TILE).T

        def narrow(ref, row, nrows):
            return halves(d, turned(ref, row, nrows, 128))[1]

        n, f = ring.at[near], ring.at[far]
        a, b = (192, 64), (256, 128)
        put(*a, 0, 128, get(n, d, *a, 0, 128) + narrow(f, 0, 128))
        x = keep(d, narrow(f, 128, 128), unpack(far, 0, True) + get(part, d, *a, 128, 128))
        put(*a, 128, 128, get(n, d, *a, 128, 128) + x)
        put(*a, 256, 128, narrow(n, 256, 128) + get(part, d, *a, 256, 128) + get(f, d, *a, 256, 128))
        put(*a, 384, 384, narrow(n, 384, 384) + get(f, d, *a, 384, 384))
        lane = lax.broadcasted_iota(jnp.int32, (128, 256), 1)
        mine = jnp.where(lane < 64 if d else lane >= 192, get(part, d, *b, 0, 256), 0.0)
        put(*b, 0, 256, get(n, d, *b, 0, 256) + turned(f, 0, 256, 256) + mine)
        top, low = (256, 64, 256, 128), (320, 64, 256, 128)
        x = keep(d, unpack(near, 1, False), halves(d, turned(n, *b, 256))[0])
        put(*top, x + get(part, d, *top) + get(f, d, *top))
        x = keep(d, halves(d, turned(f, *b, 256))[1], unpack(far, 0, False))
        put(*low, get(n, d, *low) + get(part, d, *low) + x)
        put(*b, 384, 384, turned(n, 384, 384, 256) + get(f, d, *b, 384, 384))

    def finish_end(far):
        d = 1 - far
        q = 0 if d == 0 else NZ - 1

        def put(row, nrows, col, ncols, value):
            start = (ROWS - row - nrows if d else row) - q * QR
            out[0, start:start + nrows, flip(d, col, ncols)] = value + get(part, d, row, nrows, col, ncols)

        f = ring.at[far]
        x = halves(d, get(f, d, 0, 128, 0, TILE).T)[1]
        put(64, 64, 0, TILE, keep(d, x, unpack(far, 1, True)))
        put(128, 64, 0, TILE, halves(d, get(f, d, 0, 128, 128, TILE).T)[0])

    def group2(b):
        slot = (0, 1 + last, (5 - g) // 2)[b]
        if b == 0:
            @pl.when(z == 1)
            def _():
                pack_pass(0, toward)
                pack_pass(1, away)

            @pl.when(z == 2)
            def _():
                pack_pass(1, toward)
                pack_pass(0, away)

        @pl.when(inner == 1)
        def _():
            q = mirror(1)
            for h in range(pieces(b, 1)):
                wait_far(b, 1, h)
                wait_near(b, 1, h)
                if b:
                    def body(rr, ro):
                        out[slot, ro] = ring[0, rr] + part[rr] + ring[1, rr]
                    row_loop(b, q, h * HALF, HALF, body)

        if b == 0:
            @pl.when(z == 1)
            def _():
                finish_inner(1, 0, 1)

            @pl.when(z == 2)
            def _():
                finish_inner(2, 1, 0)

        @pl.when(inner == 0)
        def _():
            q = mirror(0)

            def add_out(piece):
                start, size, cs = part_of(b, 1 - side, piece)

                def body(rr, ro):
                    out[slot, ro, cs] = ring[1 - side, rr, cs] + part[rr, cs]
                row_loop(b, q, start, size, body)

            for h in range(pieces(b, 3)):
                wait_far(b, 0, h)
                add_out(piece_of(b, 3, h))

        if b == 0:
            @pl.when(z == 0)
            def _():
                pack_copy(1, toward).wait_recv()
                finish_end(1)

            @pl.when(z == 3)
            def _():
                pack_copy(0, toward).wait_recv()
                finish_end(0)

        if b == 1:
            @pl.when(last == 1)
            def _():
                hand_over().start()

    def fill(value):
        @pl.loop(0, QR // 16)
        def _(r):
            rs = pl.ds(pl.multiple_of(r * 16, 16), 16)
            out[2, rs] = value(rs)

    start()
    compute(0, 1, NZ)

    @pl.when(z == 0)
    def _():
        pack_end(0)

    @pl.when(z == 3)
    def _():
        pack_end(1)

    @pl.when(g == 2)
    def _():
        @pl.loop(0, NZ)
        def _(i):
            q = order(i)
            arrival(1, q).wait_recv()
            row_copy(abuf.at[1], 2, q, NG - 1).start()

    group1(0)
    compute(1, 0, 3)
    group2(0)
    group1(1)
    compute(1, 3, NZ)

    @pl.when(has3 == 1)
    def _():
        compute(2, 0, 3)

    group2(1)

    @pl.when(has3 == 1)
    def _():
        group1(2)
        compute(2, 3, NZ)
        group2(2)

    @pl.when(g == 0)
    def _():
        hand_over().wait_recv()
        fill(lambda rs: got[rs])

    def drain_rows(ref):
        return pltpu.make_async_remote_copy(ref, ref, a_send, a_recv.at[0, 0],
                                            device_id={"g": (g + 1) % NG}, device_id_type=MESH)

    @pl.when(g == 2)
    def _():
        drain_rows(abuf).wait_send()

    @pl.when(g != 2)
    def _():
        drain_rows(abuf.at[0]).wait_send()

    @pl.when(last == 1)
    def _():
        hand_over().wait_send()

    @pl.when(g >= 2)
    def _():
        fill(lambda rs: jnp.zeros((16, ROWS), jnp.float32))

    packed = TILE * TILE
    first = (elements(SENT[3] + SENT[2] + SENT[1]) + packed, elements(2 * SENT[3] + SENT[2]) + 2 * packed)
    for i in range(2):
        for k in range(2):
            @pl.when((inner == i) & (has3 == k))
            def _():
                total = first[i] + (1 + k) * 3 * QR * ROWS
                ref = ring.at[:, pl.ds(0, total // 1024), pl.ds(0, 512)]
                pltpu.make_async_remote_copy(ref, ref, z_send, z_recv.at[0],
                                             device_id={"kk": toward}, device_id_type=MESH).wait_send()


def solution(mesh):
    def local_fn(a_blk):
        cols = a_blk.shape[1]
        dma = pltpu.SemaphoreType.DMA
        out = pl.pallas_call(
            kernel,
            out_shape=jax.ShapeDtypeStruct((3, QR, ROWS), jnp.float32),
            in_specs=[pl.BlockSpec(memory_space=pltpu.HBM)],
            out_specs=pl.BlockSpec(memory_space=pltpu.VMEM),
            scratch_shapes=[
                pltpu.VMEM((3, ROWS, cols), jnp.bfloat16),
                pltpu.VMEM((3 * ROWS, ROWS), jnp.float32),
                pltpu.VMEM((2, 3 * ROWS, ROWS), jnp.float32),
                pltpu.VMEM((QR, ROWS), jnp.float32),
                pltpu.VMEM((2, TILE, TILE), jnp.float32),
                pltpu.VMEM((2, TILE, TILE), jnp.float32),
                dma((2,)), dma, dma((2, NZ)), dma, dma((NRECV,)), dma((2,)), dma, dma,
            ],
            compiler_params=pltpu.CompilerParams(
                collective_id=0, has_side_effects=True, vmem_limit_bytes=50 * 2**20),
        )(a_blk)
        return out[None]

    return jax.shard_map(local_fn, mesh=mesh, in_specs=(P(("m", "g"), "kk"),),
                         out_specs=P(("m", "g"), None, "kk", None), check_vma=False)
```

```python
import jax
import jax.numpy as jnp
from jax import lax
from jax.experimental import pallas as pl
from jax.experimental.pallas import tpu as pltpu
from jax.sharding import PartitionSpec as P

MESH = pl.DeviceIdType.MESH
NZ = 4
NG = 4
ROWS = 768
QR = ROWS // NZ
HALF = QR // 2
FIRST = 256
TILE = 128
SENT = {
    3: ((64, 128, 512, TILE), (0, QR, 0, 512)),
    2: ((0, QR, 0, 384), (128, 64, 384, TILE)),
    1: ((0, QR, 0, 256),),
}
TILES = (256, 384, 512, 640)
PACK = 64 * len(TILES) + 8


def pieces(b, mq):
    return 2 if b else len(SENT[mq])


def near_index(b, mq, h):
    base = 0
    for k in range(b):
        base += sum(pieces(k, m) for m in (3, 2, 1)) + pieces(k, 3) + pieces(k, 2)
    return base + sum(pieces(b, m) for m in (3, 2, 1) if m > mq) + h


def far_index(b, mq, h):
    return near_index(b, 0, 0) + (pieces(b, 3) if mq else 0) + h


NRECV = near_index(3, 3, 0)


def elements(parts):
    return sum(p[1] * p[3] for p in parts)


def kernel(a_hbm, out, abuf, part, ring, got, pack_in, pack_out, load_sem, a_send, a_recv, z_send, z_recv,
           p_send, p_recv, t_send, t_recv):
    z = lax.axis_index("kk")
    g = lax.axis_index("g")
    side = z // 2
    inner = ((z + 1) // 2) % 2
    has3 = g % 2
    last = g // 3
    toward = z + 1 - 2 * side
    away = z - 1 + 2 * side

    def mirror(q):
        return q + side * (3 - 2 * q)

    def order(i):
        return mirror(3 - i + inner * (i // 2) * (2 * i - 5))

    def load(k):
        size = (FIRST, ROWS - FIRST)[k]
        start = ((1 - side) * (ROWS - FIRST), side * FIRST)[k]
        rs = pl.ds(pl.multiple_of(start, FIRST), size)
        return pltpu.make_async_copy(a_hbm.at[rs], abuf.at[0, rs], load_sem.at[k])

    load(0).start()
    load(1).start()

    bar = pltpu.get_barrier_semaphore()
    for d in (1, NG - 1):
        pl.semaphore_signal(bar, inc=1, device_id={"g": (g + d) % NG}, device_id_type=MESH)
    pl.semaphore_signal(bar, inc=1, device_id={"kk": toward}, device_id_type=MESH)

    @pl.when(inner == 1)
    def _():
        pl.semaphore_signal(bar, inc=1, device_id={"kk": away}, device_id_type=MESH)

    def chunk(q):
        return pl.ds(pl.multiple_of(q * QR, QR), QR)

    def row_copy(src, slot, q, d):
        return pltpu.make_async_remote_copy(
            src.at[chunk(q)], abuf.at[slot, chunk(q)], a_send, a_recv.at[slot - 1, q],
            device_id={"g": (g + d) % NG}, device_id_type=MESH)

    def arrival(slot, q):
        return row_copy(a_hbm, slot, q, NG - 1)

    def dot(x, y):
        return lax.dot_general(x, y, (((1,), (1,)), ((), ())), preferred_element_type=jnp.float32)

    def at(b, q, start, size):
        return pl.ds(pl.multiple_of(b * ROWS + q * QR + start, 16), size)

    def product(b, q):
        left = (0, 1 + last, 2 - last)[b]
        right = (0, last, 0)[b]
        part[at(b, q, 0, QR)] = dot(abuf[left, chunk(q)], abuf[right])

    def part_of(b, d, piece):
        if b:
            return piece * HALF, HALF, pl.ds(0, ROWS)
        row, nrows, col, ncols = piece
        row = row + d * (QR - 2 * row - nrows)
        col = col + d * (ROWS - 2 * col - ncols)
        return row, nrows, pl.ds(pl.multiple_of(col, 128), ncols)

    def piece_of(b, mq, h):
        return h if b else SENT[mq][h]

    def z_copy(src, b, d, piece, q, dev, index):
        start, size, cs = part_of(b, d, piece)
        return pltpu.make_async_remote_copy(
            src.at[at(b, q, start, size), cs], ring.at[d, at(b, q, start, size), cs],
            z_send, z_recv.at[index], device_id={"kk": dev}, device_id_type=MESH)

    def near_copy(src, b, mq, h, index):
        return z_copy(src, b, side, piece_of(b, mq, h), mirror(mq), toward, index)

    def far_copy(b, mq, h):
        d = 1 - side
        return z_copy(ring.at[d], b, d, piece_of(b, 3 - mq, h), mirror(mq), away, far_index(b, mq, h))

    def wait_near(b, mq, h):
        near_copy(part, b, mq, h, near_index(b, mq, h)).wait_recv()

    def wait_far(b, mq, h):
        far_copy(b, mq, h).wait_recv()

    def send_near(b, mq):
        for h in range(pieces(b, mq)):
            near_copy(part, b, mq, h, near_index(b, mq, h)).start()

    def start():
        q = order(0)
        cs = pl.ds(pl.multiple_of((1 - side) * (ROWS - FIRST), FIRST), FIRST)
        load(0).wait()
        part[at(0, q, 0, QR), cs] = dot(abuf[0, chunk(q)], abuf[0, cs])
        pl.semaphore_wait(bar, 3 + inner)

        @pl.when(inner == 0)
        def _():
            near_copy(part, 0, 3, 0, near_index(0, 3, 0)).start()

        @pl.loop(0, NZ)
        def _(i):
            row_copy(a_hbm, 1, order(i), NG - 1).start()

        @pl.when(g == 2)
        def _():
            @pl.loop(0, NZ)
            def _(i):
                row_copy(a_hbm, 2, order(i), 1).start()

        cs = pl.ds(pl.multiple_of(side * FIRST, FIRST), ROWS - FIRST)
        load(1).wait()
        part[at(0, q, 0, QR), cs] = dot(abuf[0, chunk(q)], abuf[0, cs])

        @pl.when(inner == 0)
        def _():
            near_copy(part, 0, 3, 1, near_index(0, 3, 1)).start()

    def compute(b, first, stop):
        def step(i):
            q = order(i)
            if b == 1:
                @pl.when(g < 2)
                def _():
                    arrival(1, q).wait_recv()

                @pl.when(last == 1)
                def _():
                    arrival(2, q).wait_recv()
            if b == 2:
                @pl.when(g == 1)
                def _():
                    arrival(2, q).wait_recv()
            product(b, q)
            for k in range(first, min(stop, 3)):
                @pl.when((inner == 0) & (i == k))
                def _():
                    send_near(b, 3 - k)

        if b == 1 and first == 0:
            @pl.when(last == 1)
            def _():
                for q in range(NZ):
                    arrival(1, q).wait_recv()
        pl.loop(first, stop)(step)

    def row_loop(b, q, start, size, body):
        @pl.loop(0, size // 16)
        def _(r):
            body(at(b, q, start + r * 16, 16), pl.ds(pl.multiple_of(start + r * 16, 16), 16))

    def add_in(b, d, mq, q, h):
        start, size, cs = part_of(b, d, piece_of(b, mq, h))

        def body(rr, _):
            ring[d, rr, cs] = ring[d, rr, cs] + part[rr, cs]
        row_loop(b, q, start, size, body)

    def group1(b):
        if b == 0:
            turns = ((3, 0), (0, 0), (3, 1), (2, 0), (2, 1), (0, 1))
        else:
            turns = ((3, 0), (3, 1), (0, 0), (2, 0), (0, 1), (2, 1))

        @pl.when(inner == 1)
        def _():
            for mq, h in turns:
                if mq:
                    wait_near(b, mq, h)
                    add_in(b, side, mq, mirror(mq), h)
                    near_copy(ring.at[side], b, mq, h, far_index(b, 3 - mq, h)).start()
                else:
                    wait_far(b, 0, h)
                    add_in(b, 1 - side, 3, mirror(0), h)
                    far_copy(b, 0, h).start()

    def hand_over():
        return pltpu.make_async_remote_copy(
            out.at[2], got, t_send, t_recv, device_id={"g": (g + 1) % NG}, device_id_type=MESH)

    def flip(d, start, size):
        return pl.ds(ROWS - start - size if d else start, size)

    def get(ref, d, row, nrows, col, ncols):
        return ref[flip(d, row, nrows), flip(d, col, ncols)]

    def roll(x):
        return pltpu.roll(x, 64, 1)

    def masks(d):
        row = lax.broadcasted_iota(jnp.int32, (64, TILE), 0)
        lane = lax.broadcasted_iota(jnp.int32, (64, TILE), 1)
        if d:
            return (lane >= 64) | (row > lane), row == lane
        return (lane < 64) | (row < lane - 64), row == lane - 64

    def halves(d, x):
        return (x[64:], x[:64]) if d else (x[:64], x[64:])

    def pack(d):
        plain, diagonal = masks(d)
        body, rows = [], []
        for row in TILES:
            first, second = halves(d, get(part, d, row, TILE, row, TILE))
            body.append(jnp.where(plain, second, roll(first)))
            rows.append(jnp.sum(jnp.where(diagonal, second, 0.0), axis=0, keepdims=True))
        return jnp.concatenate(body + rows + [jnp.zeros((4, TILE), jnp.float32)], axis=0)

    def unpack(d, k):
        plain, diagonal = masks(d)
        row = lax.broadcasted_iota(jnp.int32, (64, TILE), 0)
        lane = lax.broadcasted_iota(jnp.int32, (64, TILE), 1)
        x = pack_in[d, k * 64:k * 64 + 64]
        y = roll(x)
        turned = jnp.concatenate([x, y] if d else [y, x], axis=0).T
        first, second = halves(d, turned)
        second = jnp.where(plain, x, jnp.where(diagonal, pack_in[d, PACK - 8 + k:PACK - 7 + k], second))
        own = (lane >= 64) & (row <= lane - 64) if d else (lane < 64) & (row >= lane)
        first = jnp.where(own, y, first)
        return jnp.concatenate([second, first] if d else [first, second], axis=0)

    def pack_copy(d, dev):
        return pltpu.make_async_remote_copy(
            pack_out.at[d], pack_in.at[d], p_send.at[d], p_recv.at[d], device_id={"kk": dev}, device_id_type=MESH)

    def pack_end(d):
        pack_out[d] = pack(d)
        pack_copy(d, toward).start()

    def pack_pass(d, dev):
        pack_copy(d, dev).wait_recv()
        pack_out[d] = pack_in[d] + pack(d)
        pack_copy(d, dev).start()

    def finish_inner(q, near, far):
        d = near

        def put(row, nrows, col, ncols, value):
            start = (ROWS - row - nrows if d else row) - q * QR
            out[0, start:start + nrows, flip(d, col, ncols)] = value

        def turned(ref, row, nrows, col):
            return get(ref, d, row, nrows, col, TILE).T

        def narrow(ref, row, nrows):
            return halves(d, turned(ref, row, nrows, 128))[1]

        n, f = ring.at[near], ring.at[far]
        a, b = (192, 64), (256, 128)
        put(*a, 0, 128, get(n, d, *a, 0, 128) + narrow(f, 0, 128))
        x = halves(d, unpack(far, 2))[1]
        put(*a, 128, 128, get(n, d, *a, 128, 128) + get(part, d, *a, 128, 128) + x)
        put(*a, 256, 128, narrow(n, 256, 128) + get(part, d, *a, 256, 128) + get(f, d, *a, 256, 128))
        put(*a, 384, 384, narrow(n, 384, 384) + get(f, d, *a, 384, 384))
        lane = lax.broadcasted_iota(jnp.int32, (128, 256), 1)
        mine = jnp.where(lane < 64 if d else lane >= 192, get(part, d, *b, 0, 256), 0.0)
        put(*b, 0, 256, get(n, d, *b, 0, 256) + turned(f, 0, 256, 256) + mine)
        put(*b, 256, 128, unpack(near, 0) + get(part, d, *b, 256, 128) + unpack(far, 1))
        put(*b, 384, 384, turned(n, 384, 384, 256) + get(f, d, *b, 384, 384))

    def finish_end(far):
        d = 1 - far
        q = 0 if d == 0 else NZ - 1

        def put(row, nrows, col, ncols, value):
            start = (ROWS - row - nrows if d else row) - q * QR
            out[0, start:start + nrows, flip(d, col, ncols)] = value + get(part, d, row, nrows, col, ncols)

        f = ring.at[far]
        put(0, 128, 0, TILE, unpack(far, 3))
        put(128, 64, 0, TILE, halves(d, get(f, d, 0, 128, 128, TILE).T)[0])
        put(128, 64, 128, TILE, halves(d, unpack(far, 2))[0])

    def group2(b):
        slot = (0, 1 + last, (5 - g) // 2)[b]
        if b == 0:
            @pl.when(z == 1)
            def _():
                pack_pass(0, toward)
                pack_pass(1, away)

            @pl.when(z == 2)
            def _():
                pack_pass(1, toward)
                pack_pass(0, away)

        @pl.when(inner == 1)
        def _():
            q = mirror(1)
            for h in range(2):
                if h < pieces(b, 2):
                    wait_far(b, 1, h)
                if h < pieces(b, 1):
                    wait_near(b, 1, h)
                if b:
                    def body(rr, ro):
                        out[slot, ro] = ring[0, rr] + part[rr] + ring[1, rr]
                    row_loop(b, q, h * HALF, HALF, body)

        if b == 0:
            @pl.when(z == 1)
            def _():
                finish_inner(1, 0, 1)

            @pl.when(z == 2)
            def _():
                finish_inner(2, 1, 0)

        @pl.when(inner == 0)
        def _():
            q = mirror(0)

            def add_out(piece):
                start, size, cs = part_of(b, 1 - side, piece)

                def body(rr, ro):
                    out[slot, ro, cs] = ring[1 - side, rr, cs] + part[rr, cs]
                row_loop(b, q, start, size, body)

            for h in range(pieces(b, 3)):
                wait_far(b, 0, h)
                add_out(piece_of(b, 3, h))

        if b == 0:
            @pl.when(z == 0)
            def _():
                pack_copy(1, toward).wait_recv()
                finish_end(1)

            @pl.when(z == 3)
            def _():
                pack_copy(0, toward).wait_recv()
                finish_end(0)

        if b == 1:
            @pl.when(last == 1)
            def _():
                hand_over().start()

    def fill(value):
        @pl.loop(0, QR // 16)
        def _(r):
            rs = pl.ds(pl.multiple_of(r * 16, 16), 16)
            out[2, rs] = value(rs)

    start()
    compute(0, 1, NZ)

    @pl.when(z == 0)
    def _():
        pack_end(0)

    @pl.when(z == 3)
    def _():
        pack_end(1)

    @pl.when(g == 2)
    def _():
        @pl.loop(0, NZ)
        def _(i):
            q = order(i)
            arrival(1, q).wait_recv()
            row_copy(abuf.at[1], 2, q, NG - 1).start()

    group1(0)
    compute(1, 0, 3)
    group2(0)
    group1(1)
    compute(1, 3, NZ)

    @pl.when(has3 == 1)
    def _():
        compute(2, 0, 3)

    group2(1)

    @pl.when(has3 == 1)
    def _():
        group1(2)
        compute(2, 3, NZ)
        group2(2)

    @pl.when(g == 0)
    def _():
        hand_over().wait_recv()
        fill(lambda rs: got[rs])

    def drain_rows(ref):
        return pltpu.make_async_remote_copy(ref, ref, a_send, a_recv.at[0, 0],
                                            device_id={"g": (g + 1) % NG}, device_id_type=MESH)

    @pl.when(g == 2)
    def _():
        drain_rows(abuf).wait_send()

    @pl.when(g != 2)
    def _():
        drain_rows(abuf.at[0]).wait_send()

    @pl.when(last == 1)
    def _():
        hand_over().wait_send()

    @pl.when(g >= 2)
    def _():
        fill(lambda rs: jnp.zeros((16, ROWS), jnp.float32))

    pack_copy(side, toward).wait_send()

    @pl.when(inner == 1)
    def _():
        pack_copy(1 - side, toward).wait_send()

    first = (elements(SENT[3] + SENT[2] + SENT[1]), elements(2 * SENT[3] + SENT[2]))
    for i in range(2):
        for k in range(2):
            @pl.when((inner == i) & (has3 == k))
            def _():
                total = first[i] + (1 + k) * 3 * QR * ROWS
                ref = ring.at[:, pl.ds(0, total // 1024), pl.ds(0, 512)]
                pltpu.make_async_remote_copy(ref, ref, z_send, z_recv.at[0],
                                             device_id={"kk": toward}, device_id_type=MESH).wait_send()


def solution(mesh):
    def local_fn(a_blk):
        cols = a_blk.shape[1]
        dma = pltpu.SemaphoreType.DMA
        out = pl.pallas_call(
            kernel,
            out_shape=jax.ShapeDtypeStruct((3, QR, ROWS), jnp.float32),
            in_specs=[pl.BlockSpec(memory_space=pltpu.HBM)],
            out_specs=pl.BlockSpec(memory_space=pltpu.VMEM),
            scratch_shapes=[
                pltpu.VMEM((3, ROWS, cols), jnp.bfloat16),
                pltpu.VMEM((3 * ROWS, ROWS), jnp.float32),
                pltpu.VMEM((2, 3 * ROWS, ROWS), jnp.float32),
                pltpu.VMEM((QR, ROWS), jnp.float32),
                pltpu.VMEM((2, PACK, TILE), jnp.float32),
                pltpu.VMEM((2, PACK, TILE), jnp.float32),
                dma((2,)), dma, dma((2, NZ)), dma, dma((NRECV,)), dma((2,)), dma((2,)), dma, dma,
            ],
            compiler_params=pltpu.CompilerParams(
                collective_id=0, has_side_effects=True, vmem_limit_bytes=50 * 2**20),
        )(a_blk)
        return out[None]

    return jax.shard_map(local_fn, mesh=mesh, in_specs=(P(("m", "g"), "kk"),),
                         out_specs=P(("m", "g"), None, "kk", None), check_vma=False)
```

```python
import jax
import jax.numpy as jnp
from jax import lax
from jax.experimental import pallas as pl
from jax.experimental.pallas import tpu as pltpu
from jax.sharding import PartitionSpec as P

MESH = pl.DeviceIdType.MESH
NZ = 4
NG = 4
ROWS = 768
QR = ROWS // NZ
HALF = QR // 2
FIRST = 256
TILE = 128
SENT = {
    3: ((64, 128, 512, TILE), (0, QR, 0, 512)),
    2: ((0, QR, 0, 384), (128, 64, 384, TILE)),
    1: ((0, QR, 0, 256),),
}
TILES = (256, 384, 512, 640)
PACK = 64 * len(TILES) + 8


def pieces(b, mq):
    return (len(SENT[mq]), 1, 2)[b]


def near_index(b, mq, h):
    base = 0
    for k in range(b):
        base += sum(pieces(k, m) for m in (3, 2, 1)) + pieces(k, 3) + pieces(k, 2)
    return base + sum(pieces(b, m) for m in (3, 2, 1) if m > mq) + h


def far_index(b, mq, h):
    return near_index(b, 0, 0) + (pieces(b, 3) if mq else 0) + h


NRECV = near_index(3, 3, 0)


def elements(parts):
    return sum(p[1] * p[3] for p in parts)


def kernel(a_hbm, out, abuf, part, ring, got, pack_in, pack_out, load_sem, a_send, a_recv, z_send, z_recv,
           p_send, p_recv, t_send, t_recv):
    z = lax.axis_index("kk")
    g = lax.axis_index("g")
    side = z // 2
    inner = ((z + 1) // 2) % 2
    has3 = g % 2
    last = g // 3
    toward = z + 1 - 2 * side
    away = z - 1 + 2 * side

    def mirror(q):
        return q + side * (3 - 2 * q)

    def order(i):
        return mirror(3 - i + inner * (i // 2) * (2 * i - 5))

    def load(k):
        size = (FIRST, ROWS - FIRST)[k]
        start = ((1 - side) * (ROWS - FIRST), side * FIRST)[k]
        rs = pl.ds(pl.multiple_of(start, FIRST), size)
        return pltpu.make_async_copy(a_hbm.at[rs], abuf.at[0, rs], load_sem.at[k])

    load(0).start()
    load(1).start()

    bar = pltpu.get_barrier_semaphore()
    for d in (1, NG - 1):
        pl.semaphore_signal(bar, inc=1, device_id={"g": (g + d) % NG}, device_id_type=MESH)
    pl.semaphore_signal(bar, inc=1, device_id={"kk": toward}, device_id_type=MESH)

    @pl.when(inner == 1)
    def _():
        pl.semaphore_signal(bar, inc=1, device_id={"kk": away}, device_id_type=MESH)

    def chunk(q):
        return pl.ds(pl.multiple_of(q * QR, QR), QR)

    def row_copy(src, slot, q, d):
        return pltpu.make_async_remote_copy(
            src.at[chunk(q)], abuf.at[slot, chunk(q)], a_send, a_recv.at[slot - 1, q],
            device_id={"g": (g + d) % NG}, device_id_type=MESH)

    def arrival(slot, q):
        return row_copy(a_hbm, slot, q, NG - 1)

    def dot(x, y):
        return lax.dot_general(x, y, (((1,), (1,)), ((), ())), preferred_element_type=jnp.float32)

    def at(b, q, start, size):
        return pl.ds(pl.multiple_of(b * ROWS + q * QR + start, 16), size)

    def product(b, q):
        left = (0, 1 + last, 2 - last)[b]
        right = (0, last, 0)[b]
        part[at(b, q, 0, QR)] = dot(abuf[left, chunk(q)], abuf[right])

    def part_of(b, d, piece):
        if b:
            size = QR // pieces(b, 3)
            return piece * size, size, pl.ds(0, ROWS)
        row, nrows, col, ncols = piece
        row = row + d * (QR - 2 * row - nrows)
        col = col + d * (ROWS - 2 * col - ncols)
        return row, nrows, pl.ds(pl.multiple_of(col, 128), ncols)

    def piece_of(b, mq, h):
        return h if b else SENT[mq][h]

    def z_copy(src, b, d, piece, q, dev, index):
        start, size, cs = part_of(b, d, piece)
        return pltpu.make_async_remote_copy(
            src.at[at(b, q, start, size), cs], ring.at[d, at(b, q, start, size), cs],
            z_send, z_recv.at[index], device_id={"kk": dev}, device_id_type=MESH)

    def near_copy(src, b, mq, h, index):
        return z_copy(src, b, side, piece_of(b, mq, h), mirror(mq), toward, index)

    def far_copy(b, mq, h):
        d = 1 - side
        return z_copy(ring.at[d], b, d, piece_of(b, 3 - mq, h), mirror(mq), away, far_index(b, mq, h))

    def wait_near(b, mq, h):
        near_copy(part, b, mq, h, near_index(b, mq, h)).wait_recv()

    def wait_far(b, mq, h):
        far_copy(b, mq, h).wait_recv()

    def send_near(b, mq):
        for h in range(pieces(b, mq)):
            near_copy(part, b, mq, h, near_index(b, mq, h)).start()

    def start():
        q = order(0)
        cs = pl.ds(pl.multiple_of((1 - side) * (ROWS - FIRST), FIRST), FIRST)
        load(0).wait()
        part[at(0, q, 0, QR), cs] = dot(abuf[0, chunk(q)], abuf[0, cs])
        pl.semaphore_wait(bar, 3 + inner)

        @pl.when(inner == 0)
        def _():
            near_copy(part, 0, 3, 0, near_index(0, 3, 0)).start()

        @pl.loop(0, NZ)
        def _(i):
            row_copy(a_hbm, 1, order(i), NG - 1).start()

        @pl.when(g == 2)
        def _():
            @pl.loop(0, NZ)
            def _(i):
                row_copy(a_hbm, 2, order(i), 1).start()

        cs = pl.ds(pl.multiple_of(side * FIRST, FIRST), ROWS - FIRST)
        load(1).wait()
        part[at(0, q, 0, QR), cs] = dot(abuf[0, chunk(q)], abuf[0, cs])

        @pl.when(inner == 0)
        def _():
            near_copy(part, 0, 3, 1, near_index(0, 3, 1)).start()

    def compute(b, first, stop):
        def step(i):
            q = order(i)
            if b == 1:
                @pl.when(g < 2)
                def _():
                    arrival(1, q).wait_recv()

                @pl.when(last == 1)
                def _():
                    arrival(2, q).wait_recv()
            if b == 2:
                @pl.when(g == 1)
                def _():
                    arrival(2, q).wait_recv()
            product(b, q)
            for k in range(first, min(stop, 3)):
                @pl.when((inner == 0) & (i == k))
                def _():
                    send_near(b, 3 - k)

        if b == 1 and first == 0:
            @pl.when(last == 1)
            def _():
                for q in range(NZ):
                    arrival(1, q).wait_recv()
        pl.loop(first, stop)(step)

    def row_loop(b, q, start, size, body):
        @pl.loop(0, size // 16)
        def _(r):
            body(at(b, q, start + r * 16, 16), pl.ds(pl.multiple_of(start + r * 16, 16), 16))

    def add_in(b, d, mq, q, h):
        start, size, cs = part_of(b, d, piece_of(b, mq, h))

        def body(rr, _):
            ring[d, rr, cs] = ring[d, rr, cs] + part[rr, cs]
        row_loop(b, q, start, size, body)

    def group1(b):
        turns = (((3, 0), (0, 0), (3, 1), (2, 0), (2, 1), (0, 1)),
                 ((3, 0), (2, 0), (0, 0)),
                 ((3, 0), (3, 1), (0, 0), (2, 0), (0, 1), (2, 1)))[b]

        @pl.when(inner == 1)
        def _():
            for mq, h in turns:
                if mq:
                    wait_near(b, mq, h)
                    add_in(b, side, mq, mirror(mq), h)
                    near_copy(ring.at[side], b, mq, h, far_index(b, 3 - mq, h)).start()
                else:
                    wait_far(b, 0, h)
                    add_in(b, 1 - side, 3, mirror(0), h)
                    far_copy(b, 0, h).start()

    def hand_over():
        return pltpu.make_async_remote_copy(
            out.at[2], got, t_send, t_recv, device_id={"g": (g + 1) % NG}, device_id_type=MESH)

    def flip(d, start, size):
        return pl.ds(ROWS - start - size if d else start, size)

    def get(ref, d, row, nrows, col, ncols):
        return ref[flip(d, row, nrows), flip(d, col, ncols)]

    def roll(x):
        return pltpu.roll(x, 64, 1)

    def masks(d):
        row = lax.broadcasted_iota(jnp.int32, (64, TILE), 0)
        lane = lax.broadcasted_iota(jnp.int32, (64, TILE), 1)
        if d:
            return (lane >= 64) | (row > lane), row == lane
        return (lane < 64) | (row < lane - 64), row == lane - 64

    def halves(d, x):
        return (x[64:], x[:64]) if d else (x[:64], x[64:])

    def pack(d):
        plain, diagonal = masks(d)
        body, rows = [], []
        for row in TILES:
            first, second = halves(d, get(part, d, row, TILE, row, TILE))
            body.append(jnp.where(plain, second, roll(first)))
            rows.append(jnp.sum(jnp.where(diagonal, second, 0.0), axis=0, keepdims=True))
        return jnp.concatenate(body + rows + [jnp.zeros((4, TILE), jnp.float32)], axis=0)

    def unpack(d, k):
        plain, diagonal = masks(d)
        row = lax.broadcasted_iota(jnp.int32, (64, TILE), 0)
        lane = lax.broadcasted_iota(jnp.int32, (64, TILE), 1)
        x = pack_in[d, k * 64:k * 64 + 64]
        y = roll(x)
        turned = jnp.concatenate([x, y] if d else [y, x], axis=0).T
        first, second = halves(d, turned)
        second = jnp.where(plain, x, jnp.where(diagonal, pack_in[d, PACK - 8 + k:PACK - 7 + k], second))
        own = (lane >= 64) & (row <= lane - 64) if d else (lane < 64) & (row >= lane)
        first = jnp.where(own, y, first)
        return jnp.concatenate([second, first] if d else [first, second], axis=0)

    def pack_copy(d, dev):
        return pltpu.make_async_remote_copy(
            pack_out.at[d], pack_in.at[d], p_send.at[d], p_recv.at[d], device_id={"kk": dev}, device_id_type=MESH)

    def pack_end(d):
        pack_out[d] = pack(d)
        pack_copy(d, toward).start()

    def pack_pass(d, dev):
        pack_copy(d, dev).wait_recv()
        pack_out[d] = pack_in[d] + pack(d)
        pack_copy(d, dev).start()

    def finish_inner(q, near, far):
        d = near

        def put(row, nrows, col, ncols, value):
            start = (ROWS - row - nrows if d else row) - q * QR
            out[0, start:start + nrows, flip(d, col, ncols)] = value

        def turned(ref, row, nrows, col):
            return get(ref, d, row, nrows, col, TILE).T

        def narrow(ref, row, nrows):
            return halves(d, turned(ref, row, nrows, 128))[1]

        n, f = ring.at[near], ring.at[far]
        a, b = (192, 64), (256, 128)
        put(*a, 0, 128, get(n, d, *a, 0, 128) + narrow(f, 0, 128))
        x = halves(d, unpack(far, 2))[1]
        put(*a, 128, 128, get(n, d, *a, 128, 128) + get(part, d, *a, 128, 128) + x)
        put(*a, 256, 128, narrow(n, 256, 128) + get(part, d, *a, 256, 128) + get(f, d, *a, 256, 128))
        put(*a, 384, 384, narrow(n, 384, 384) + get(f, d, *a, 384, 384))
        lane = lax.broadcasted_iota(jnp.int32, (128, 256), 1)
        mine = jnp.where(lane < 64 if d else lane >= 192, get(part, d, *b, 0, 256), 0.0)
        put(*b, 0, 256, get(n, d, *b, 0, 256) + turned(f, 0, 256, 256) + mine)
        put(*b, 256, 128, unpack(near, 0) + get(part, d, *b, 256, 128) + unpack(far, 1))
        put(*b, 384, 384, turned(n, 384, 384, 256) + get(f, d, *b, 384, 384))

    def finish_end(far):
        d = 1 - far
        q = 0 if d == 0 else NZ - 1

        def put(row, nrows, col, ncols, value):
            start = (ROWS - row - nrows if d else row) - q * QR
            out[0, start:start + nrows, flip(d, col, ncols)] = value + get(part, d, row, nrows, col, ncols)

        f = ring.at[far]
        put(0, 128, 0, TILE, unpack(far, 3))
        put(128, 64, 0, TILE, halves(d, get(f, d, 0, 128, 128, TILE).T)[0])
        put(128, 64, 128, TILE, halves(d, unpack(far, 2))[0])

    def group2(b):
        slot = (0, 1 + last, (5 - g) // 2)[b]
        if b == 0:
            @pl.when(z == 1)
            def _():
                pack_pass(0, toward)
                pack_pass(1, away)

            @pl.when(z == 2)
            def _():
                pack_pass(1, toward)
                pack_pass(0, away)

        @pl.when(inner == 1)
        def _():
            q = mirror(1)
            for h in range(2):
                if h < pieces(b, 2):
                    wait_far(b, 1, h)
                if h < pieces(b, 1):
                    wait_near(b, 1, h)
                if b and h < pieces(b, 1):
                    def body(rr, ro):
                        out[slot, ro] = ring[0, rr] + part[rr] + ring[1, rr]
                    row_loop(b, q, *part_of(b, 0, h)[:2], body)

        if b == 0:
            @pl.when(z == 1)
            def _():
                finish_inner(1, 0, 1)

            @pl.when(z == 2)
            def _():
                finish_inner(2, 1, 0)

        @pl.when(inner == 0)
        def _():
            q = mirror(0)

            def add_out(piece):
                start, size, cs = part_of(b, 1 - side, piece)

                def body(rr, ro):
                    out[slot, ro, cs] = ring[1 - side, rr, cs] + part[rr, cs]
                row_loop(b, q, start, size, body)

            for h in range(pieces(b, 3)):
                wait_far(b, 0, h)
                add_out(piece_of(b, 3, h))

        if b == 0:
            @pl.when(z == 0)
            def _():
                pack_copy(1, toward).wait_recv()
                finish_end(1)

            @pl.when(z == 3)
            def _():
                pack_copy(0, toward).wait_recv()
                finish_end(0)

        if b == 1:
            @pl.when(last == 1)
            def _():
                hand_over().start()

    def fill(value):
        @pl.loop(0, QR // 16)
        def _(r):
            rs = pl.ds(pl.multiple_of(r * 16, 16), 16)
            out[2, rs] = value(rs)

    start()
    compute(0, 1, NZ)

    @pl.when(z == 0)
    def _():
        pack_end(0)

    @pl.when(z == 3)
    def _():
        pack_end(1)

    @pl.when(g == 2)
    def _():
        @pl.loop(0, NZ)
        def _(i):
            q = order(i)
            arrival(1, q).wait_recv()
            row_copy(abuf.at[1], 2, q, NG - 1).start()

    group1(0)
    compute(1, 0, 3)
    group2(0)
    group1(1)
    compute(1, 3, NZ)

    @pl.when(has3 == 1)
    def _():
        compute(2, 0, 3)

    group2(1)

    @pl.when(has3 == 1)
    def _():
        group1(2)
        compute(2, 3, NZ)

    def drain_rows(ref):
        return pltpu.make_async_remote_copy(ref, ref, a_send, a_recv.at[0, 0],
                                            device_id={"g": (g + 1) % NG}, device_id_type=MESH)

    @pl.when(g == 2)
    def _():
        drain_rows(abuf).wait_send()

    @pl.when(g != 2)
    def _():
        drain_rows(abuf.at[0]).wait_send()

    @pl.when(last == 1)
    def _():
        hand_over().wait_send()

    @pl.when(g >= 2)
    def _():
        fill(lambda rs: jnp.zeros((16, ROWS), jnp.float32))

    pack_copy(side, toward).wait_send()

    @pl.when(inner == 1)
    def _():
        pack_copy(1 - side, toward).wait_send()

    @pl.when(has3 == 1)
    def _():
        group2(2)

    @pl.when(g == 0)
    def _():
        hand_over().wait_recv()
        fill(lambda rs: got[rs])

    first = (elements(SENT[3] + SENT[2] + SENT[1]), elements(2 * SENT[3] + SENT[2]))
    for i in range(2):
        for k in range(2):
            @pl.when((inner == i) & (has3 == k))
            def _():
                total = first[i] + (1 + k) * 3 * QR * ROWS
                ref = ring.at[:, pl.ds(0, total // 1024), pl.ds(0, 512)]
                pltpu.make_async_remote_copy(ref, ref, z_send, z_recv.at[0],
                                             device_id={"kk": toward}, device_id_type=MESH).wait_send()


def solution(mesh):
    def local_fn(a_blk):
        cols = a_blk.shape[1]
        dma = pltpu.SemaphoreType.DMA
        out = pl.pallas_call(
            kernel,
            out_shape=jax.ShapeDtypeStruct((3, QR, ROWS), jnp.float32),
            in_specs=[pl.BlockSpec(memory_space=pltpu.HBM)],
            out_specs=pl.BlockSpec(memory_space=pltpu.VMEM),
            scratch_shapes=[
                pltpu.VMEM((3, ROWS, cols), jnp.bfloat16),
                pltpu.VMEM((3 * ROWS, ROWS), jnp.float32),
                pltpu.VMEM((2, 3 * ROWS, ROWS), jnp.float32),
                pltpu.VMEM((QR, ROWS), jnp.float32),
                pltpu.VMEM((2, PACK, TILE), jnp.float32),
                pltpu.VMEM((2, PACK, TILE), jnp.float32),
                dma((2,)), dma, dma((2, NZ)), dma, dma((NRECV,)), dma((2,)), dma((2,)), dma, dma,
            ],
            compiler_params=pltpu.CompilerParams(
                collective_id=0, has_side_effects=True, vmem_limit_bytes=50 * 2**20),
        )(a_blk)
        return out[None]

    return jax.shard_map(local_fn, mesh=mesh, in_specs=(P(("m", "g"), "kk"),),
                         out_specs=P(("m", "g"), None, "kk", None), check_vma=False)
```

```python
import jax
import jax.numpy as jnp
from jax import lax
from jax.experimental import pallas as pl
from jax.experimental.pallas import tpu as pltpu
from jax.sharding import PartitionSpec as P

MESH = pl.DeviceIdType.MESH
NZ = 4
NG = 4
ROWS = 768
QR = ROWS // NZ
HALF = QR // 2
FIRST = 256
TILE = 128
SENT = {
    3: ((64, 128, 512, TILE), (0, QR, 0, 512)),
    2: ((0, QR, 0, 384), (128, 64, 384, TILE)),
    1: ((0, QR, 0, 256),),
}
TILES = (256, 384, 512, 640)
PACK = 64 * len(TILES) + 8


def pieces(b, mq):
    return (len(SENT[mq]), 1, 2)[b]


def near_index(b, mq, h):
    if b == 0:
        return 0 if mq == 3 else 1
    base = 4 if b == 1 else 4 + sum(pieces(1, m) for m in (3, 2, 1, 3, 2))
    return base + sum(pieces(b, m) for m in (3, 2, 1) if m > mq) + h


def far_index(b, mq, h):
    if b == 0:
        return 2 + mq
    return near_index(b, 0, 0) + (pieces(b, 3) if mq else 0) + h


NRECV = far_index(2, 1, pieces(2, 2))


def elements(parts):
    return sum(p[1] * p[3] for p in parts)


def kernel(a_hbm, out, abuf, part, ring, got, pack_in, pack_out, load_sem, a_send, a_recv, z_send, z_recv,
           p_send, p_recv, t_send, t_recv):
    z = lax.axis_index("kk")
    g = lax.axis_index("g")
    side = z // 2
    inner = ((z + 1) // 2) % 2
    has3 = g % 2
    last = g // 3
    toward = z + 1 - 2 * side
    away = z - 1 + 2 * side

    def mirror(q):
        return q + side * (3 - 2 * q)

    def order(i):
        return mirror(3 - i + inner * (i // 2) * (2 * i - 5))

    def load(k):
        size = (FIRST, ROWS - FIRST)[k]
        start = ((1 - side) * (ROWS - FIRST), side * FIRST)[k]
        rs = pl.ds(pl.multiple_of(start, FIRST), size)
        return pltpu.make_async_copy(a_hbm.at[rs], abuf.at[0, rs], load_sem.at[k])

    load(0).start()
    load(1).start()

    bar = pltpu.get_barrier_semaphore()
    for d in (1, NG - 1):
        pl.semaphore_signal(bar, inc=1, device_id={"g": (g + d) % NG}, device_id_type=MESH)
    pl.semaphore_signal(bar, inc=1, device_id={"kk": toward}, device_id_type=MESH)

    @pl.when(inner == 1)
    def _():
        pl.semaphore_signal(bar, inc=1, device_id={"kk": away}, device_id_type=MESH)

    def chunk(q):
        return pl.ds(pl.multiple_of(q * QR, QR), QR)

    def row_copy(src, slot, q, d):
        return pltpu.make_async_remote_copy(
            src.at[chunk(q)], abuf.at[slot, chunk(q)], a_send, a_recv.at[slot - 1, q],
            device_id={"g": (g + d) % NG}, device_id_type=MESH)

    def arrival(slot, q):
        return row_copy(a_hbm, slot, q, NG - 1)

    def dot(x, y):
        return lax.dot_general(x, y, (((1,), (1,)), ((), ())), preferred_element_type=jnp.float32)

    def at(b, q, start, size):
        return pl.ds(pl.multiple_of(b * ROWS + q * QR + start, 16), size)

    def product(b, q):
        left = (0, 1 + last, 2 - last)[b]
        right = (0, last, 0)[b]
        part[at(b, q, 0, QR)] = dot(abuf[left, chunk(q)], abuf[right])

    def part_of(b, d, piece):
        if b:
            size = QR // pieces(b, 3)
            return piece * size, size, pl.ds(0, ROWS)
        row, nrows, col, ncols = piece
        row = row + d * (QR - 2 * row - nrows)
        col = col + d * (ROWS - 2 * col - ncols)
        return row, nrows, pl.ds(pl.multiple_of(col, 128), ncols)

    def piece_of(b, mq, h):
        return h if b else SENT[mq][h]

    def z_copy(src, b, d, piece, q, dev, index):
        start, size, cs = part_of(b, d, piece)
        return pltpu.make_async_remote_copy(
            src.at[at(b, q, start, size), cs], ring.at[d, at(b, q, start, size), cs],
            z_send, z_recv.at[index], device_id={"kk": dev}, device_id_type=MESH)

    def near_copy(src, b, mq, h, index):
        return z_copy(src, b, side, piece_of(b, mq, h), mirror(mq), toward, index)

    def far_copy(b, mq, h):
        d = 1 - side
        return z_copy(ring.at[d], b, d, piece_of(b, 3 - mq, h), mirror(mq), away, far_index(b, mq, h))

    def wait_all(index, parts):
        ref = ring.at[:, pl.ds(0, elements(parts) // 1024), pl.ds(0, 512)]
        pltpu.make_async_remote_copy(ref, ref, z_send, z_recv.at[index], device_id={"kk": toward},
                                     device_id_type=MESH).wait_recv()

    def wait_near(b, mq, h):
        if b:
            near_copy(part, b, mq, h, near_index(b, mq, h)).wait_recv()
        elif h == 0 and mq > 1:
            wait_all(near_index(0, mq, 0), SENT[3] if mq == 3 else SENT[2] + SENT[1])

    def wait_far(b, mq, h):
        if b:
            far_copy(b, mq, h).wait_recv()
        elif h == 0:
            wait_all(far_index(0, mq, 0), SENT[3 - mq])

    def send_near(b, mq):
        for h in range(pieces(b, mq)):
            near_copy(part, b, mq, h, near_index(b, mq, h)).start()

    def start():
        q = order(0)
        cs = pl.ds(pl.multiple_of((1 - side) * (ROWS - FIRST), FIRST), FIRST)
        load(0).wait()
        part[at(0, q, 0, QR), cs] = dot(abuf[0, chunk(q)], abuf[0, cs])
        pl.semaphore_wait(bar, 3 + inner)

        @pl.when(inner == 0)
        def _():
            near_copy(part, 0, 3, 0, near_index(0, 3, 0)).start()

        @pl.loop(0, NZ)
        def _(i):
            row_copy(a_hbm, 1, order(i), NG - 1).start()

        @pl.when(g == 2)
        def _():
            @pl.loop(0, NZ)
            def _(i):
                row_copy(a_hbm, 2, order(i), 1).start()

        cs = pl.ds(pl.multiple_of(side * FIRST, FIRST), ROWS - FIRST)
        load(1).wait()
        part[at(0, q, 0, QR), cs] = dot(abuf[0, chunk(q)], abuf[0, cs])

        @pl.when(inner == 0)
        def _():
            near_copy(part, 0, 3, 1, near_index(0, 3, 1)).start()

    def compute(b, first, stop):
        def step(i):
            q = order(i)
            if b == 1:
                @pl.when(g < 2)
                def _():
                    arrival(1, q).wait_recv()

                @pl.when(last == 1)
                def _():
                    arrival(2, q).wait_recv()
            if b == 2:
                @pl.when(g == 1)
                def _():
                    arrival(2, q).wait_recv()
            product(b, q)
            for k in range(first, min(stop, 3)):
                @pl.when((inner == 0) & (i == k))
                def _():
                    send_near(b, 3 - k)

        if b == 1 and first == 0:
            @pl.when(last == 1)
            def _():
                for q in range(NZ):
                    arrival(1, q).wait_recv()
        pl.loop(first, stop)(step)

    def row_loop(b, q, start, size, body):
        @pl.loop(0, size // 16)
        def _(r):
            body(at(b, q, start + r * 16, 16), pl.ds(pl.multiple_of(start + r * 16, 16), 16))

    def add_in(b, d, mq, q, h):
        start, size, cs = part_of(b, d, piece_of(b, mq, h))

        def body(rr, _):
            ring[d, rr, cs] = ring[d, rr, cs] + part[rr, cs]
        row_loop(b, q, start, size, body)

    def group1(b):
        turns = (((3, 0), (3, 1), (2, 0), (2, 1), (0, 0), (0, 1)),
                 ((3, 0), (2, 0), (0, 0)),
                 ((3, 0), (3, 1), (0, 0), (2, 0), (0, 1), (2, 1)))[b]

        @pl.when(inner == 1)
        def _():
            for mq, h in turns:
                if mq:
                    wait_near(b, mq, h)
                    add_in(b, side, mq, mirror(mq), h)
                    near_copy(ring.at[side], b, mq, h, far_index(b, 3 - mq, h)).start()
                else:
                    wait_far(b, 0, h)
                    add_in(b, 1 - side, 3, mirror(0), h)
                    far_copy(b, 0, h).start()

    def hand_over():
        return pltpu.make_async_remote_copy(
            out.at[2], got, t_send, t_recv, device_id={"g": (g + 1) % NG}, device_id_type=MESH)

    def flip(d, start, size):
        return pl.ds(ROWS - start - size if d else start, size)

    def get(ref, d, row, nrows, col, ncols):
        return ref[flip(d, row, nrows), flip(d, col, ncols)]

    def roll(x):
        return pltpu.roll(x, 64, 1)

    def masks(d):
        row = lax.broadcasted_iota(jnp.int32, (64, TILE), 0)
        lane = lax.broadcasted_iota(jnp.int32, (64, TILE), 1)
        if d:
            return (lane >= 64) | (row > lane), row == lane
        return (lane < 64) | (row < lane - 64), row == lane - 64

    def halves(d, x):
        return (x[64:], x[:64]) if d else (x[:64], x[64:])

    def pack(d):
        plain, diagonal = masks(d)
        body, rows = [], []
        for row in TILES:
            first, second = halves(d, get(part, d, row, TILE, row, TILE))
            body.append(jnp.where(plain, second, roll(first)))
            rows.append(jnp.sum(jnp.where(diagonal, second, 0.0), axis=0, keepdims=True))
        return jnp.concatenate(body + rows + [jnp.zeros((4, TILE), jnp.float32)], axis=0)

    def unpack(d, k):
        plain, diagonal = masks(d)
        row = lax.broadcasted_iota(jnp.int32, (64, TILE), 0)
        lane = lax.broadcasted_iota(jnp.int32, (64, TILE), 1)
        x = pack_in[d, k * 64:k * 64 + 64]
        y = roll(x)
        turned = jnp.concatenate([x, y] if d else [y, x], axis=0).T
        first, second = halves(d, turned)
        second = jnp.where(plain, x, jnp.where(diagonal, pack_in[d, PACK - 8 + k:PACK - 7 + k], second))
        own = (lane >= 64) & (row <= lane - 64) if d else (lane < 64) & (row >= lane)
        first = jnp.where(own, y, first)
        return jnp.concatenate([second, first] if d else [first, second], axis=0)

    def pack_copy(d, dev):
        return pltpu.make_async_remote_copy(
            pack_out.at[d], pack_in.at[d], p_send, p_recv.at[d], device_id={"kk": dev}, device_id_type=MESH)

    def pack_end(d):
        pack_out[d] = pack(d)
        pack_copy(d, toward).start()

    def pack_pass(d, dev):
        pack_copy(d, dev).wait_recv()
        pack_out[d] = pack_in[d] + pack(d)
        pack_copy(d, dev).start()

    def finish_inner(q, near, far):
        d = near

        def put(row, nrows, col, ncols, value):
            start = (ROWS - row - nrows if d else row) - q * QR
            out[0, start:start + nrows, flip(d, col, ncols)] = value

        def turned(ref, row, nrows, col):
            return get(ref, d, row, nrows, col, TILE).T

        def narrow(ref, row, nrows):
            return halves(d, turned(ref, row, nrows, 128))[1]

        n, f = ring.at[near], ring.at[far]
        a, b = (192, 64), (256, 128)
        put(*a, 0, 128, get(n, d, *a, 0, 128) + narrow(f, 0, 128))
        x = halves(d, unpack(far, 2))[1]
        put(*a, 128, 128, get(n, d, *a, 128, 128) + get(part, d, *a, 128, 128) + x)
        put(*a, 256, 128, narrow(n, 256, 128) + get(part, d, *a, 256, 128) + get(f, d, *a, 256, 128))
        put(*a, 384, 384, narrow(n, 384, 384) + get(f, d, *a, 384, 384))
        lane = lax.broadcasted_iota(jnp.int32, (128, 256), 1)
        mine = jnp.where(lane < 64 if d else lane >= 192, get(part, d, *b, 0, 256), 0.0)
        put(*b, 0, 256, get(n, d, *b, 0, 256) + turned(f, 0, 256, 256) + mine)
        put(*b, 256, 128, unpack(near, 0) + get(part, d, *b, 256, 128) + unpack(far, 1))
        put(*b, 384, 384, turned(n, 384, 384, 256) + get(f, d, *b, 384, 384))

    def finish_end(far):
        d = 1 - far
        q = 0 if d == 0 else NZ - 1

        def put(row, nrows, col, ncols, value):
            start = (ROWS - row - nrows if d else row) - q * QR
            out[0, start:start + nrows, flip(d, col, ncols)] = value + get(part, d, row, nrows, col, ncols)

        f = ring.at[far]
        put(0, 128, 0, TILE, unpack(far, 3))
        put(128, 64, 0, TILE, halves(d, get(f, d, 0, 128, 128, TILE).T)[0])
        put(128, 64, 128, TILE, halves(d, unpack(far, 2))[0])

    def group2(b):
        slot = (0, 1 + last, (5 - g) // 2)[b]
        if b == 0:
            @pl.when(z == 1)
            def _():
                pack_pass(0, toward)
                pack_pass(1, away)

            @pl.when(z == 2)
            def _():
                pack_pass(1, toward)
                pack_pass(0, away)

        @pl.when(inner == 1)
        def _():
            q = mirror(1)
            for h in range(2):
                if h < pieces(b, 2):
                    wait_far(b, 1, h)
                if h < pieces(b, 1):
                    wait_near(b, 1, h)
                if b and h < pieces(b, 1):
                    def body(rr, ro):
                        out[slot, ro] = ring[0, rr] + part[rr] + ring[1, rr]
                    row_loop(b, q, *part_of(b, 0, h)[:2], body)

        if b == 0:
            @pl.when(z == 1)
            def _():
                finish_inner(1, 0, 1)

            @pl.when(z == 2)
            def _():
                finish_inner(2, 1, 0)

        @pl.when(inner == 0)
        def _():
            q = mirror(0)

            def add_out(piece):
                start, size, cs = part_of(b, 1 - side, piece)

                def body(rr, ro):
                    out[slot, ro, cs] = ring[1 - side, rr, cs] + part[rr, cs]
                row_loop(b, q, start, size, body)

            for h in range(pieces(b, 3)):
                wait_far(b, 0, h)
                add_out(piece_of(b, 3, h))

        if b == 0:
            @pl.when(z == 0)
            def _():
                pack_copy(1, toward).wait_recv()
                finish_end(1)

            @pl.when(z == 3)
            def _():
                pack_copy(0, toward).wait_recv()
                finish_end(0)

        if b == 1:
            @pl.when(last == 1)
            def _():
                hand_over().start()

    def fill(value):
        @pl.loop(0, QR // 16)
        def _(r):
            rs = pl.ds(pl.multiple_of(r * 16, 16), 16)
            out[2, rs] = value(rs)

    start()
    compute(0, 1, NZ)

    @pl.when(z == 0)
    def _():
        pack_end(0)

    @pl.when(z == 3)
    def _():
        pack_end(1)

    @pl.when(g == 2)
    def _():
        @pl.loop(0, NZ)
        def _(i):
            q = order(i)
            arrival(1, q).wait_recv()
            row_copy(abuf.at[1], 2, q, NG - 1).start()

    group1(0)
    compute(1, 0, 3)
    group2(0)
    group1(1)
    compute(1, 3, NZ)

    @pl.when(has3 == 1)
    def _():
        compute(2, 0, 3)

    group2(1)

    @pl.when(has3 == 1)
    def _():
        group1(2)
        compute(2, 3, NZ)

    def drain_rows(ref):
        return pltpu.make_async_remote_copy(ref, ref, a_send, a_recv.at[0, 0],
                                            device_id={"g": (g + 1) % NG}, device_id_type=MESH)

    @pl.when(g == 2)
    def _():
        drain_rows(abuf).wait_send()

    @pl.when(g != 2)
    def _():
        drain_rows(abuf.at[0]).wait_send()

    @pl.when(last == 1)
    def _():
        hand_over().wait_send()

    @pl.when(g >= 2)
    def _():
        fill(lambda rs: jnp.zeros((16, ROWS), jnp.float32))

    @pl.when(inner == 0)
    def _():
        pack_copy(side, toward).wait_send()

    @pl.when(inner == 1)
    def _():
        pltpu.make_async_remote_copy(pack_out, pack_in, p_send, p_recv.at[0], device_id={"kk": toward},
                                     device_id_type=MESH).wait_send()

    @pl.when(has3 == 1)
    def _():
        group2(2)

    @pl.when(g == 0)
    def _():
        hand_over().wait_recv()
        fill(lambda rs: got[rs])

    first = (elements(SENT[3] + SENT[2] + SENT[1]), elements(2 * SENT[3] + SENT[2]))
    for i in range(2):
        for k in range(2):
            @pl.when((inner == i) & (has3 == k))
            def _():
                total = first[i] + (1 + k) * 3 * QR * ROWS
                ref = ring.at[:, pl.ds(0, total // 1024), pl.ds(0, 512)]
                pltpu.make_async_remote_copy(ref, ref, z_send, z_recv.at[0],
                                             device_id={"kk": toward}, device_id_type=MESH).wait_send()


def solution(mesh):
    def local_fn(a_blk):
        cols = a_blk.shape[1]
        dma = pltpu.SemaphoreType.DMA
        out = pl.pallas_call(
            kernel,
            out_shape=jax.ShapeDtypeStruct((3, QR, ROWS), jnp.float32),
            in_specs=[pl.BlockSpec(memory_space=pltpu.HBM)],
            out_specs=pl.BlockSpec(memory_space=pltpu.VMEM),
            scratch_shapes=[
                pltpu.VMEM((3, ROWS, cols), jnp.bfloat16),
                pltpu.VMEM((3 * ROWS, ROWS), jnp.float32),
                pltpu.VMEM((2, 3 * ROWS, ROWS), jnp.float32),
                pltpu.VMEM((QR, ROWS), jnp.float32),
                pltpu.VMEM((2, PACK, TILE), jnp.float32),
                pltpu.VMEM((2, PACK, TILE), jnp.float32),
                dma((2,)), dma, dma((2, NZ)), dma, dma((NRECV,)), dma, dma((2,)), dma, dma,
            ],
            compiler_params=pltpu.CompilerParams(
                collective_id=0, has_side_effects=True, vmem_limit_bytes=50 * 2**20),
        )(a_blk)
        return out[None]

    return jax.shard_map(local_fn, mesh=mesh, in_specs=(P(("m", "g"), "kk"),),
                         out_specs=P(("m", "g"), None, "kk", None), check_vma=False)
```

```python
import jax
import jax.numpy as jnp
from jax import lax
from jax.experimental import pallas as pl
from jax.experimental.pallas import tpu as pltpu
from jax.sharding import PartitionSpec as P

MESH = pl.DeviceIdType.MESH
NZ = 4
NG = 4
ROWS = 768
QR = ROWS // NZ
HALF = QR // 2
FIRST = 256
TILE = 128
SENT = {
    3: ((64, 128, 512, TILE), (0, QR, 0, 512)),
    2: ((0, QR, 0, 384), (128, 64, 384, TILE)),
    1: ((0, QR, 0, 256),),
}
TILES = (256, 384, 512, 640)
PACK = 64 * len(TILES) + 8


def pieces(b, mq):
    return (len(SENT[mq]), 1, 2)[b]


def near_index(b, mq, h):
    if b == 0:
        return 0 if mq == 3 else 1
    base = 4 if b == 1 else 4 + sum(pieces(1, m) for m in (3, 2, 1, 3, 2))
    return base + sum(pieces(b, m) for m in (3, 2, 1) if m > mq) + h


def far_index(b, mq, h):
    if b == 0:
        return 2 + mq
    return near_index(b, 0, 0) + (pieces(b, 3) if mq else 0) + h


NRECV = far_index(2, 1, pieces(2, 2))


def elements(parts):
    return sum(p[1] * p[3] for p in parts)


def kernel(a_hbm, out, abuf, part, ring, got, pack_in, pack_out, load_sem, a_send, a_recv, z_send, z_recv,
           p_send, p_recv, t_send, t_recv):
    z = lax.axis_index("kk")
    g = lax.axis_index("g")
    side = z // 2
    inner = ((z + 1) // 2) % 2
    has3 = g % 2
    last = g // 3
    toward = z + 1 - 2 * side
    away = z - 1 + 2 * side

    def mirror(q):
        return q + side * (3 - 2 * q)

    def order(i):
        return mirror(3 - i + inner * (i // 2) * (2 * i - 5))

    def load(k):
        size = (FIRST, ROWS - FIRST)[k]
        start = ((1 - side) * (ROWS - FIRST), side * FIRST)[k]
        rs = pl.ds(pl.multiple_of(start, FIRST), size)
        return pltpu.make_async_copy(a_hbm.at[rs], abuf.at[0, rs], load_sem.at[k])

    load(0).start()
    load(1).start()

    bar = pltpu.get_barrier_semaphore()
    for d in (1, NG - 1):
        pl.semaphore_signal(bar, inc=1, device_id={"g": (g + d) % NG}, device_id_type=MESH)
    pl.semaphore_signal(bar, inc=1, device_id={"kk": toward}, device_id_type=MESH)

    @pl.when(inner == 1)
    def _():
        pl.semaphore_signal(bar, inc=1, device_id={"kk": away}, device_id_type=MESH)

    def chunk(q):
        return pl.ds(pl.multiple_of(q * QR, QR), QR)

    def row_copy(src, slot, q, d):
        return pltpu.make_async_remote_copy(
            src.at[chunk(q)], abuf.at[slot, chunk(q)], a_send, a_recv.at[slot - 1, q],
            device_id={"g": (g + d) % NG}, device_id_type=MESH)

    def arrival(slot, q):
        return row_copy(a_hbm, slot, q, NG - 1)

    def dot(x, y):
        return lax.dot_general(x, y, (((1,), (1,)), ((), ())), preferred_element_type=jnp.float32)

    def at(b, q, start, size):
        return pl.ds(pl.multiple_of(b * ROWS + q * QR + start, 16), size)

    def product(b, q):
        left = (0, 1 + last, 2 - last)[b]
        right = (0, last, 0)[b]
        part[at(b, q, 0, QR)] = dot(abuf[left, chunk(q)], abuf[right])

    def part_of(b, d, piece):
        if b:
            size = QR // pieces(b, 3)
            return piece * size, size, pl.ds(0, ROWS)
        row, nrows, col, ncols = piece
        row = row + d * (QR - 2 * row - nrows)
        col = col + d * (ROWS - 2 * col - ncols)
        return row, nrows, pl.ds(pl.multiple_of(col, 128), ncols)

    def piece_of(b, mq, h):
        return h if b else SENT[mq][h]

    def z_copy(src, b, d, piece, q, dev, index):
        start, size, cs = part_of(b, d, piece)
        return pltpu.make_async_remote_copy(
            src.at[at(b, q, start, size), cs], ring.at[d, at(b, q, start, size), cs],
            z_send, z_recv.at[index], device_id={"kk": dev}, device_id_type=MESH)

    def near_copy(src, b, mq, h, index):
        return z_copy(src, b, side, piece_of(b, mq, h), mirror(mq), toward, index)

    def far_copy(b, mq, h):
        d = 1 - side
        return z_copy(ring.at[d], b, d, piece_of(b, 3 - mq, h), mirror(mq), away, far_index(b, mq, h))

    def wait_all(index, parts):
        ref = ring.at[:, pl.ds(0, elements(parts) // 1024), pl.ds(0, 512)]
        pltpu.make_async_remote_copy(ref, ref, z_send, z_recv.at[index], device_id={"kk": toward},
                                     device_id_type=MESH).wait_recv()

    def wait_near(b, mq, h):
        if b:
            near_copy(part, b, mq, h, near_index(b, mq, h)).wait_recv()
        elif h == 0 and mq > 1:
            wait_all(near_index(0, mq, 0), SENT[3] if mq == 3 else SENT[2] + SENT[1])

    def wait_far(b, mq, h):
        if b:
            far_copy(b, mq, h).wait_recv()
        elif h == 0:
            wait_all(far_index(0, mq, 0), SENT[3 - mq])

    def send_near(b, mq):
        for h in range(pieces(b, mq)):
            near_copy(part, b, mq, h, near_index(b, mq, h)).start()

    def start():
        q = order(0)
        cs = pl.ds(pl.multiple_of((1 - side) * (ROWS - FIRST), FIRST), FIRST)
        load(0).wait()
        part[at(0, q, 0, QR), cs] = dot(abuf[0, chunk(q)], abuf[0, cs])
        pl.semaphore_wait(bar, 3 + inner)

        @pl.when(inner == 0)
        def _():
            near_copy(part, 0, 3, 0, near_index(0, 3, 0)).start()

        @pl.loop(0, NZ)
        def _(i):
            row_copy(a_hbm, 1, order(i), NG - 1).start()

        @pl.when(g == 2)
        def _():
            @pl.loop(0, NZ)
            def _(i):
                row_copy(a_hbm, 2, order(i), 1).start()

        cs = pl.ds(pl.multiple_of(side * FIRST, FIRST), ROWS - FIRST)
        load(1).wait()
        part[at(0, q, 0, QR), cs] = dot(abuf[0, chunk(q)], abuf[0, cs])

        @pl.when(inner == 0)
        def _():
            near_copy(part, 0, 3, 1, near_index(0, 3, 1)).start()

    def compute(b, first, stop):
        def step(i):
            q = order(i)
            if b == 1:
                @pl.when(g < 2)
                def _():
                    arrival(1, q).wait_recv()

                @pl.when(last == 1)
                def _():
                    arrival(2, q).wait_recv()
            if b == 2:
                @pl.when(g == 1)
                def _():
                    arrival(2, q).wait_recv()
            product(b, q)
            for k in range(first, min(stop, 3)):
                @pl.when((inner == 0) & (i == k))
                def _():
                    send_near(b, 3 - k)

        if b == 1 and first == 0:
            @pl.when(last == 1)
            def _():
                for q in range(NZ):
                    arrival(1, q).wait_recv()
        pl.loop(first, stop)(step)

    def row_loop(b, q, start, size, body):
        @pl.loop(0, size // 32)
        def _(r):
            body(at(b, q, start + r * 32, 32), pl.ds(pl.multiple_of(start + r * 32, 32), 32))

    def add_in(b, d, mq, q, h):
        start, size, cs = part_of(b, d, piece_of(b, mq, h))

        def body(rr, _):
            ring[d, rr, cs] = ring[d, rr, cs] + part[rr, cs]
        row_loop(b, q, start, size, body)

    def group1(b):
        turns = (((3, 0), (3, 1), (2, 0), (2, 1), (0, 0), (0, 1)),
                 ((3, 0), (2, 0), (0, 0)),
                 ((3, 0), (3, 1), (0, 0), (2, 0), (0, 1), (2, 1)))[b]

        @pl.when(inner == 1)
        def _():
            for mq, h in turns:
                if mq:
                    wait_near(b, mq, h)
                    add_in(b, side, mq, mirror(mq), h)
                    near_copy(ring.at[side], b, mq, h, far_index(b, 3 - mq, h)).start()
                else:
                    wait_far(b, 0, h)
                    add_in(b, 1 - side, 3, mirror(0), h)
                    far_copy(b, 0, h).start()

    def hand_over():
        return pltpu.make_async_remote_copy(
            out.at[2], got, t_send, t_recv, device_id={"g": (g + 1) % NG}, device_id_type=MESH)

    def flip(d, start, size):
        return pl.ds(ROWS - start - size if d else start, size)

    def get(ref, d, row, nrows, col, ncols):
        return ref[flip(d, row, nrows), flip(d, col, ncols)]

    def roll(x):
        return pltpu.roll(x, 64, 1)

    def masks(d):
        row = lax.broadcasted_iota(jnp.int32, (64, TILE), 0)
        lane = lax.broadcasted_iota(jnp.int32, (64, TILE), 1)
        if d:
            return (lane >= 64) | (row > lane), row == lane
        return (lane < 64) | (row < lane - 64), row == lane - 64

    def halves(d, x):
        return (x[64:], x[:64]) if d else (x[:64], x[64:])

    def pack(d):
        plain, diagonal = masks(d)
        body, rows = [], []
        for row in TILES:
            first, second = halves(d, get(part, d, row, TILE, row, TILE))
            body.append(jnp.where(plain, second, roll(first)))
            rows.append(jnp.sum(jnp.where(diagonal, second, 0.0), axis=0, keepdims=True))
        return jnp.concatenate(body + rows + [jnp.zeros((4, TILE), jnp.float32)], axis=0)

    def unpack(d, k):
        plain, diagonal = masks(d)
        row = lax.broadcasted_iota(jnp.int32, (64, TILE), 0)
        lane = lax.broadcasted_iota(jnp.int32, (64, TILE), 1)
        x = pack_in[d, k * 64:k * 64 + 64]
        y = roll(x)
        turned = jnp.concatenate([x, y] if d else [y, x], axis=0).T
        first, second = halves(d, turned)
        second = jnp.where(plain, x, jnp.where(diagonal, pack_in[d, PACK - 8 + k:PACK - 7 + k], second))
        own = (lane >= 64) & (row <= lane - 64) if d else (lane < 64) & (row >= lane)
        first = jnp.where(own, y, first)
        return jnp.concatenate([second, first] if d else [first, second], axis=0)

    def pack_copy(d, dev):
        return pltpu.make_async_remote_copy(
            pack_out.at[d], pack_in.at[d], p_send, p_recv.at[d], device_id={"kk": dev}, device_id_type=MESH)

    def pack_end(d):
        pack_out[d] = pack(d)
        pack_copy(d, toward).start()

    def pack_pass(d, dev):
        pack_copy(d, dev).wait_recv()
        pack_out[d] = pack_in[d] + pack(d)
        pack_copy(d, dev).start()

    def finish_inner(q, near, far):
        d = near

        def put(row, nrows, col, ncols, value):
            start = (ROWS - row - nrows if d else row) - q * QR
            out[0, start:start + nrows, flip(d, col, ncols)] = value

        def turned(ref, row, nrows, col):
            return get(ref, d, row, nrows, col, TILE).T

        def narrow(ref, row, nrows):
            return halves(d, turned(ref, row, nrows, 128))[1]

        n, f = ring.at[near], ring.at[far]
        a, b = (192, 64), (256, 128)
        put(*a, 0, 128, get(n, d, *a, 0, 128) + narrow(f, 0, 128))
        x = halves(d, unpack(far, 2))[1]
        put(*a, 128, 128, get(n, d, *a, 128, 128) + get(part, d, *a, 128, 128) + x)
        put(*a, 256, 128, narrow(n, 256, 128) + get(part, d, *a, 256, 128) + get(f, d, *a, 256, 128))
        put(*a, 384, 384, narrow(n, 384, 384) + get(f, d, *a, 384, 384))
        lane = lax.broadcasted_iota(jnp.int32, (128, 256), 1)
        mine = jnp.where(lane < 64 if d else lane >= 192, get(part, d, *b, 0, 256), 0.0)
        put(*b, 0, 256, get(n, d, *b, 0, 256) + turned(f, 0, 256, 256) + mine)
        put(*b, 256, 128, unpack(near, 0) + get(part, d, *b, 256, 128) + unpack(far, 1))
        put(*b, 384, 384, turned(n, 384, 384, 256) + get(f, d, *b, 384, 384))

    def finish_end(far):
        d = 1 - far
        q = 0 if d == 0 else NZ - 1

        def put(row, nrows, col, ncols, value):
            start = (ROWS - row - nrows if d else row) - q * QR
            out[0, start:start + nrows, flip(d, col, ncols)] = value + get(part, d, row, nrows, col, ncols)

        f = ring.at[far]
        put(0, 128, 0, TILE, unpack(far, 3))
        put(128, 64, 0, TILE, halves(d, get(f, d, 0, 128, 128, TILE).T)[0])
        put(128, 64, 128, TILE, halves(d, unpack(far, 2))[0])

    def group2(b):
        slot = (0, 1 + last, (5 - g) // 2)[b]
        if b == 0:
            @pl.when(z == 1)
            def _():
                pack_pass(0, toward)
                pack_pass(1, away)

            @pl.when(z == 2)
            def _():
                pack_pass(1, toward)
                pack_pass(0, away)

        @pl.when(inner == 1)
        def _():
            q = mirror(1)
            for h in range(2):
                if h < pieces(b, 2):
                    wait_far(b, 1, h)
                if h < pieces(b, 1):
                    wait_near(b, 1, h)
                if b and h < pieces(b, 1):
                    def body(rr, ro):
                        out[slot, ro] = ring[0, rr] + part[rr] + ring[1, rr]
                    row_loop(b, q, *part_of(b, 0, h)[:2], body)

        if b == 0:
            @pl.when(z == 1)
            def _():
                finish_inner(1, 0, 1)

            @pl.when(z == 2)
            def _():
                finish_inner(2, 1, 0)

        @pl.when(inner == 0)
        def _():
            q = mirror(0)

            def add_out(piece):
                start, size, cs = part_of(b, 1 - side, piece)

                def body(rr, ro):
                    out[slot, ro, cs] = ring[1 - side, rr, cs] + part[rr, cs]
                row_loop(b, q, start, size, body)

            for h in range(pieces(b, 3)):
                wait_far(b, 0, h)
                add_out(piece_of(b, 3, h))

        if b == 0:
            @pl.when(z == 0)
            def _():
                pack_copy(1, toward).wait_recv()
                finish_end(1)

            @pl.when(z == 3)
            def _():
                pack_copy(0, toward).wait_recv()
                finish_end(0)

        if b == 1:
            @pl.when(last == 1)
            def _():
                hand_over().start()

    def fill(value):
        @pl.loop(0, QR // 16)
        def _(r):
            rs = pl.ds(pl.multiple_of(r * 16, 16), 16)
            out[2, rs] = value(rs)

    start()
    compute(0, 1, NZ)

    @pl.when(z == 0)
    def _():
        pack_end(0)

    @pl.when(z == 3)
    def _():
        pack_end(1)

    @pl.when(g == 2)
    def _():
        @pl.loop(0, NZ)
        def _(i):
            q = order(i)
            arrival(1, q).wait_recv()
            row_copy(abuf.at[1], 2, q, NG - 1).start()

    group1(0)
    compute(1, 0, 3)
    group2(0)
    group1(1)
    compute(1, 3, NZ)

    @pl.when(has3 == 1)
    def _():
        compute(2, 0, 3)

    group2(1)

    @pl.when(has3 == 1)
    def _():
        group1(2)
        compute(2, 3, NZ)

    def drain_rows(ref):
        return pltpu.make_async_remote_copy(ref, ref, a_send, a_recv.at[0, 0],
                                            device_id={"g": (g + 1) % NG}, device_id_type=MESH)

    @pl.when(g == 2)
    def _():
        drain_rows(abuf).wait_send()

    @pl.when(g != 2)
    def _():
        drain_rows(abuf.at[0]).wait_send()

    @pl.when(last == 1)
    def _():
        hand_over().wait_send()

    @pl.when(g >= 2)
    def _():
        fill(lambda rs: jnp.zeros((16, ROWS), jnp.float32))

    @pl.when(inner == 0)
    def _():
        pack_copy(side, toward).wait_send()

    @pl.when(inner == 1)
    def _():
        pltpu.make_async_remote_copy(pack_out, pack_in, p_send, p_recv.at[0], device_id={"kk": toward},
                                     device_id_type=MESH).wait_send()

    @pl.when(has3 == 1)
    def _():
        group2(2)

    @pl.when(g == 0)
    def _():
        hand_over().wait_recv()
        fill(lambda rs: got[rs])

    first = (elements(SENT[3] + SENT[2] + SENT[1]), elements(2 * SENT[3] + SENT[2]))
    for i in range(2):
        for k in range(2):
            @pl.when((inner == i) & (has3 == k))
            def _():
                total = first[i] + (1 + k) * 3 * QR * ROWS
                ref = ring.at[:, pl.ds(0, total // 1024), pl.ds(0, 512)]
                pltpu.make_async_remote_copy(ref, ref, z_send, z_recv.at[0],
                                             device_id={"kk": toward}, device_id_type=MESH).wait_send()


def solution(mesh):
    def local_fn(a_blk):
        cols = a_blk.shape[1]
        dma = pltpu.SemaphoreType.DMA
        out = pl.pallas_call(
            kernel,
            out_shape=jax.ShapeDtypeStruct((3, QR, ROWS), jnp.float32),
            in_specs=[pl.BlockSpec(memory_space=pltpu.HBM)],
            out_specs=pl.BlockSpec(memory_space=pltpu.VMEM),
            scratch_shapes=[
                pltpu.VMEM((3, ROWS, cols), jnp.bfloat16),
                pltpu.VMEM((3 * ROWS, ROWS), jnp.float32),
                pltpu.VMEM((2, 3 * ROWS, ROWS), jnp.float32),
                pltpu.VMEM((QR, ROWS), jnp.float32),
                pltpu.VMEM((2, PACK, TILE), jnp.float32),
                pltpu.VMEM((2, PACK, TILE), jnp.float32),
                dma((2,)), dma, dma((2, NZ)), dma, dma((NRECV,)), dma, dma((2,)), dma, dma,
            ],
            compiler_params=pltpu.CompilerParams(
                collective_id=0, has_side_effects=True, vmem_limit_bytes=50 * 2**20),
        )(a_blk)
        return out[None]

    return jax.shard_map(local_fn, mesh=mesh, in_specs=(P(("m", "g"), "kk"),),
                         out_specs=P(("m", "g"), None, "kk", None), check_vma=False)
```

```python
import jax
import jax.numpy as jnp
from jax import lax
from jax.experimental import pallas as pl
from jax.experimental.pallas import tpu as pltpu
from jax.sharding import PartitionSpec as P

MESH = pl.DeviceIdType.MESH
NZ = 4
NG = 4
ROWS = 768
QR = ROWS // NZ
HALF = QR // 2
FIRST = 256
TILE = 128
SENT = {
    3: ((64, 128, 512, TILE), (0, QR, 0, 512)),
    2: ((0, QR, 0, 384), (128, 64, 384, TILE)),
    1: ((0, QR, 0, 256),),
}
TILES = (256, 384, 512, 640)
PACK = 64 * len(TILES) + 8


def pieces(b, mq):
    return (len(SENT[mq]), 1, 2)[b]


def near_index(b, mq, h):
    if b == 0:
        return 0 if mq == 3 else 1
    base = 4 if b == 1 else 4 + sum(pieces(1, m) for m in (3, 2, 1, 3, 2))
    return base + sum(pieces(b, m) for m in (3, 2, 1) if m > mq) + h


def far_index(b, mq, h):
    if b == 0:
        return 2 + mq
    return near_index(b, 0, 0) + (pieces(b, 3) if mq else 0) + h


NRECV = far_index(2, 1, pieces(2, 2))


def elements(parts):
    return sum(p[1] * p[3] for p in parts)


def kernel(a_hbm, out, abuf, part, ring, got, pack_in, pack_out, load_sem, a_send, a_recv, z_send, z_recv,
           p_send, p_recv, t_send, t_recv):
    z = lax.axis_index("kk")
    g = lax.axis_index("g")
    side = z // 2
    inner = ((z + 1) // 2) % 2
    has3 = g % 2
    last = g // 3
    toward = z + 1 - 2 * side
    away = z - 1 + 2 * side

    def mirror(q):
        return q + side * (3 - 2 * q)

    def order(i):
        return mirror(3 - i + inner * (i // 2) * (2 * i - 5))

    def load(k):
        size = (FIRST, ROWS - FIRST)[k]
        start = ((1 - side) * (ROWS - FIRST), side * FIRST)[k]
        rs = pl.ds(pl.multiple_of(start, FIRST), size)
        return pltpu.make_async_copy(a_hbm.at[rs], abuf.at[0, rs], load_sem.at[k])

    load(0).start()
    load(1).start()

    bar = pltpu.get_barrier_semaphore()
    for d in (1, NG - 1):
        pl.semaphore_signal(bar, inc=1, device_id={"g": (g + d) % NG}, device_id_type=MESH)
    pl.semaphore_signal(bar, inc=1, device_id={"kk": toward}, device_id_type=MESH)

    @pl.when(inner == 1)
    def _():
        pl.semaphore_signal(bar, inc=1, device_id={"kk": away}, device_id_type=MESH)

    def chunk(q):
        return pl.ds(pl.multiple_of(q * QR, QR), QR)

    def row_copy(src, slot, q, d):
        return pltpu.make_async_remote_copy(
            src.at[chunk(q)], abuf.at[slot, chunk(q)], a_send, a_recv.at[slot - 1, q],
            device_id={"g": (g + d) % NG}, device_id_type=MESH)

    def arrival(slot, q):
        return row_copy(a_hbm, slot, q, NG - 1)

    def dot(x, y):
        return lax.dot_general(x, y, (((1,), (1,)), ((), ())), preferred_element_type=jnp.float32)

    def at(b, q, start, size):
        return pl.ds(pl.multiple_of(b * ROWS + q * QR + start, 16), size)

    def product(b, q):
        left = (0, 1 + last, 2 - last)[b]
        right = (0, last, 0)[b]
        part[at(b, q, 0, QR)] = dot(abuf[left, chunk(q)], abuf[right])

    def part_of(b, d, piece):
        if b:
            size = QR // pieces(b, 3)
            return piece * size, size, pl.ds(0, ROWS)
        row, nrows, col, ncols = piece
        row = row + d * (QR - 2 * row - nrows)
        col = col + d * (ROWS - 2 * col - ncols)
        return row, nrows, pl.ds(pl.multiple_of(col, 128), ncols)

    def piece_of(b, mq, h):
        return h if b else SENT[mq][h]

    def z_copy(src, b, d, piece, q, dev, index):
        start, size, cs = part_of(b, d, piece)
        return pltpu.make_async_remote_copy(
            src.at[at(b, q, start, size), cs], ring.at[d, at(b, q, start, size), cs],
            z_send, z_recv.at[index], device_id={"kk": dev}, device_id_type=MESH)

    def near_copy(src, b, mq, h, index):
        return z_copy(src, b, side, piece_of(b, mq, h), mirror(mq), toward, index)

    def far_copy(b, mq, h):
        d = 1 - side
        return z_copy(ring.at[d], b, d, piece_of(b, 3 - mq, h), mirror(mq), away, far_index(b, mq, h))

    def wait_all(index, parts):
        ref = ring.at[:, pl.ds(0, elements(parts) // 1024), pl.ds(0, 512)]
        pltpu.make_async_remote_copy(ref, ref, z_send, z_recv.at[index], device_id={"kk": toward},
                                     device_id_type=MESH).wait_recv()

    def wait_near(b, mq, h):
        if b:
            near_copy(part, b, mq, h, near_index(b, mq, h)).wait_recv()
        elif h == 0 and mq > 1:
            wait_all(near_index(0, mq, 0), SENT[3] if mq == 3 else SENT[2] + SENT[1])

    def wait_far(b, mq, h):
        if b:
            far_copy(b, mq, h).wait_recv()
        elif h == 0:
            wait_all(far_index(0, mq, 0), SENT[3 - mq])

    def send_near(b, mq):
        for h in range(pieces(b, mq)):
            near_copy(part, b, mq, h, near_index(b, mq, h)).start()

    def start():
        q = order(0)
        cs = pl.ds(pl.multiple_of((1 - side) * (ROWS - FIRST), FIRST), FIRST)
        load(0).wait()
        part[at(0, q, 0, QR), cs] = dot(abuf[0, chunk(q)], abuf[0, cs])
        pl.semaphore_wait(bar, 3 + inner)

        @pl.when(inner == 0)
        def _():
            near_copy(part, 0, 3, 0, near_index(0, 3, 0)).start()

        @pl.loop(0, NZ)
        def _(i):
            row_copy(a_hbm, 1, order(i), NG - 1).start()

        @pl.when(g == 2)
        def _():
            @pl.loop(0, NZ)
            def _(i):
                row_copy(a_hbm, 2, order(i), 1).start()

        cs = pl.ds(pl.multiple_of(side * FIRST, FIRST), ROWS - FIRST)
        load(1).wait()
        part[at(0, q, 0, QR), cs] = dot(abuf[0, chunk(q)], abuf[0, cs])

        @pl.when(inner == 0)
        def _():
            near_copy(part, 0, 3, 1, near_index(0, 3, 1)).start()

    def compute(b, first, stop):
        def step(i):
            q = order(i)
            if b == 1:
                @pl.when(g < 2)
                def _():
                    arrival(1, q).wait_recv()

                @pl.when(last == 1)
                def _():
                    arrival(2, q).wait_recv()
            if b == 2:
                @pl.when(g == 1)
                def _():
                    arrival(2, q).wait_recv()
            product(b, q)
            for k in range(first, min(stop, 3)):
                @pl.when((inner == 0) & (i == k))
                def _():
                    send_near(b, 3 - k)

        if b == 1 and first == 0:
            @pl.when(last == 1)
            def _():
                for q in range(NZ):
                    arrival(1, q).wait_recv()
        pl.loop(first, stop)(step)

    def row_loop(b, q, start, size, body):
        @pl.loop(0, size // 32, unroll=True)
        def _(r):
            body(at(b, q, start + r * 32, 32), pl.ds(pl.multiple_of(start + r * 32, 32), 32))

    def add_in(b, d, mq, q, h):
        start, size, cs = part_of(b, d, piece_of(b, mq, h))

        def body(rr, _):
            ring[d, rr, cs] = ring[d, rr, cs] + part[rr, cs]
        row_loop(b, q, start, size, body)

    def group1(b):
        turns = (((3, 0), (3, 1), (2, 0), (2, 1), (0, 0), (0, 1)),
                 ((3, 0), (2, 0), (0, 0)),
                 ((3, 0), (3, 1), (0, 0), (2, 0), (0, 1), (2, 1)))[b]

        @pl.when(inner == 1)
        def _():
            for mq, h in turns:
                if mq:
                    wait_near(b, mq, h)
                    add_in(b, side, mq, mirror(mq), h)
                    near_copy(ring.at[side], b, mq, h, far_index(b, 3 - mq, h)).start()
                else:
                    wait_far(b, 0, h)
                    add_in(b, 1 - side, 3, mirror(0), h)
                    far_copy(b, 0, h).start()

    def hand_over():
        return pltpu.make_async_remote_copy(
            out.at[2], got, t_send, t_recv, device_id={"g": (g + 1) % NG}, device_id_type=MESH)

    def flip(d, start, size):
        return pl.ds(ROWS - start - size if d else start, size)

    def get(ref, d, row, nrows, col, ncols):
        return ref[flip(d, row, nrows), flip(d, col, ncols)]

    def roll(x):
        return pltpu.roll(x, 64, 1)

    def masks(d):
        row = lax.broadcasted_iota(jnp.int32, (64, TILE), 0)
        lane = lax.broadcasted_iota(jnp.int32, (64, TILE), 1)
        if d:
            return (lane >= 64) | (row > lane), row == lane
        return (lane < 64) | (row < lane - 64), row == lane - 64

    def halves(d, x):
        return (x[64:], x[:64]) if d else (x[:64], x[64:])

    def pack(d):
        plain, diagonal = masks(d)
        body, rows = [], []
        for row in TILES:
            first, second = halves(d, get(part, d, row, TILE, row, TILE))
            body.append(jnp.where(plain, second, roll(first)))
            rows.append(jnp.sum(jnp.where(diagonal, second, 0.0), axis=0, keepdims=True))
        return jnp.concatenate(body + rows + [jnp.zeros((4, TILE), jnp.float32)], axis=0)

    def unpack(d, k):
        plain, diagonal = masks(d)
        row = lax.broadcasted_iota(jnp.int32, (64, TILE), 0)
        lane = lax.broadcasted_iota(jnp.int32, (64, TILE), 1)
        x = pack_in[d, k * 64:k * 64 + 64]
        y = roll(x)
        turned = jnp.concatenate([x, y] if d else [y, x], axis=0).T
        first, second = halves(d, turned)
        second = jnp.where(plain, x, jnp.where(diagonal, pack_in[d, PACK - 8 + k:PACK - 7 + k], second))
        own = (lane >= 64) & (row <= lane - 64) if d else (lane < 64) & (row >= lane)
        first = jnp.where(own, y, first)
        return jnp.concatenate([second, first] if d else [first, second], axis=0)

    def pack_copy(d, dev):
        return pltpu.make_async_remote_copy(
            pack_out.at[d], pack_in.at[d], p_send, p_recv.at[d], device_id={"kk": dev}, device_id_type=MESH)

    def pack_end(d):
        pack_out[d] = pack(d)
        pack_copy(d, toward).start()

    def pack_pass(d, dev):
        pack_copy(d, dev).wait_recv()
        pack_out[d] = pack_in[d] + pack(d)
        pack_copy(d, dev).start()

    def finish_inner(q, near, far):
        d = near

        def put(row, nrows, col, ncols, value):
            start = (ROWS - row - nrows if d else row) - q * QR
            out[0, start:start + nrows, flip(d, col, ncols)] = value

        def turned(ref, row, nrows, col):
            return get(ref, d, row, nrows, col, TILE).T

        def narrow(ref, row, nrows):
            return halves(d, turned(ref, row, nrows, 128))[1]

        n, f = ring.at[near], ring.at[far]
        a, b = (192, 64), (256, 128)
        put(*a, 0, 128, get(n, d, *a, 0, 128) + narrow(f, 0, 128))
        x = halves(d, unpack(far, 2))[1]
        put(*a, 128, 128, get(n, d, *a, 128, 128) + get(part, d, *a, 128, 128) + x)
        put(*a, 256, 128, narrow(n, 256, 128) + get(part, d, *a, 256, 128) + get(f, d, *a, 256, 128))
        put(*a, 384, 384, narrow(n, 384, 384) + get(f, d, *a, 384, 384))
        lane = lax.broadcasted_iota(jnp.int32, (128, 256), 1)
        mine = jnp.where(lane < 64 if d else lane >= 192, get(part, d, *b, 0, 256), 0.0)
        put(*b, 0, 256, get(n, d, *b, 0, 256) + turned(f, 0, 256, 256) + mine)
        put(*b, 256, 128, unpack(near, 0) + get(part, d, *b, 256, 128) + unpack(far, 1))
        put(*b, 384, 384, turned(n, 384, 384, 256) + get(f, d, *b, 384, 384))

    def finish_end(far):
        d = 1 - far
        q = 0 if d == 0 else NZ - 1

        def put(row, nrows, col, ncols, value):
            start = (ROWS - row - nrows if d else row) - q * QR
            out[0, start:start + nrows, flip(d, col, ncols)] = value + get(part, d, row, nrows, col, ncols)

        f = ring.at[far]
        put(0, 128, 0, TILE, unpack(far, 3))
        put(128, 64, 0, TILE, halves(d, get(f, d, 0, 128, 128, TILE).T)[0])
        put(128, 64, 128, TILE, halves(d, unpack(far, 2))[0])

    def group2(b):
        slot = (0, 1 + last, (5 - g) // 2)[b]
        if b == 0:
            @pl.when(z == 1)
            def _():
                pack_pass(0, toward)
                pack_pass(1, away)

            @pl.when(z == 2)
            def _():
                pack_pass(1, toward)
                pack_pass(0, away)

        @pl.when(inner == 1)
        def _():
            q = mirror(1)
            for h in range(2):
                if h < pieces(b, 2):
                    wait_far(b, 1, h)
                if h < pieces(b, 1):
                    wait_near(b, 1, h)
                if b and h < pieces(b, 1):
                    def body(rr, ro):
                        out[slot, ro] = ring[0, rr] + part[rr] + ring[1, rr]
                    row_loop(b, q, *part_of(b, 0, h)[:2], body)

        if b == 0:
            @pl.when(z == 1)
            def _():
                finish_inner(1, 0, 1)

            @pl.when(z == 2)
            def _():
                finish_inner(2, 1, 0)

        @pl.when(inner == 0)
        def _():
            q = mirror(0)

            def add_out(piece):
                start, size, cs = part_of(b, 1 - side, piece)

                def body(rr, ro):
                    out[slot, ro, cs] = ring[1 - side, rr, cs] + part[rr, cs]
                row_loop(b, q, start, size, body)

            for h in range(pieces(b, 3)):
                wait_far(b, 0, h)
                add_out(piece_of(b, 3, h))

        if b == 0:
            @pl.when(z == 0)
            def _():
                pack_copy(1, toward).wait_recv()
                finish_end(1)

            @pl.when(z == 3)
            def _():
                pack_copy(0, toward).wait_recv()
                finish_end(0)

        if b == 1:
            @pl.when(last == 1)
            def _():
                hand_over().start()

    def fill(value):
        @pl.loop(0, QR // 16)
        def _(r):
            rs = pl.ds(pl.multiple_of(r * 16, 16), 16)
            out[2, rs] = value(rs)

    start()
    compute(0, 1, NZ)

    @pl.when(z == 0)
    def _():
        pack_end(0)

    @pl.when(z == 3)
    def _():
        pack_end(1)

    @pl.when(g == 2)
    def _():
        @pl.loop(0, NZ)
        def _(i):
            q = order(i)
            arrival(1, q).wait_recv()
            row_copy(abuf.at[1], 2, q, NG - 1).start()

    group1(0)
    compute(1, 0, 3)
    group2(0)
    group1(1)
    compute(1, 3, NZ)

    @pl.when(has3 == 1)
    def _():
        compute(2, 0, 3)

    group2(1)

    @pl.when(has3 == 1)
    def _():
        group1(2)
        compute(2, 3, NZ)

    def drain_rows(ref):
        return pltpu.make_async_remote_copy(ref, ref, a_send, a_recv.at[0, 0],
                                            device_id={"g": (g + 1) % NG}, device_id_type=MESH)

    @pl.when(g == 2)
    def _():
        drain_rows(abuf).wait_send()

    @pl.when(g != 2)
    def _():
        drain_rows(abuf.at[0]).wait_send()

    @pl.when(last == 1)
    def _():
        hand_over().wait_send()

    @pl.when(g >= 2)
    def _():
        fill(lambda rs: jnp.zeros((16, ROWS), jnp.float32))

    @pl.when(inner == 0)
    def _():
        pack_copy(side, toward).wait_send()

    @pl.when(inner == 1)
    def _():
        pltpu.make_async_remote_copy(pack_out, pack_in, p_send, p_recv.at[0], device_id={"kk": toward},
                                     device_id_type=MESH).wait_send()

    @pl.when(has3 == 1)
    def _():
        group2(2)

    @pl.when(g == 0)
    def _():
        hand_over().wait_recv()
        fill(lambda rs: got[rs])

    first = (elements(SENT[3] + SENT[2] + SENT[1]), elements(2 * SENT[3] + SENT[2]))
    for i in range(2):
        for k in range(2):
            @pl.when((inner == i) & (has3 == k))
            def _():
                total = first[i] + (1 + k) * 3 * QR * ROWS
                ref = ring.at[:, pl.ds(0, total // 1024), pl.ds(0, 512)]
                pltpu.make_async_remote_copy(ref, ref, z_send, z_recv.at[0],
                                             device_id={"kk": toward}, device_id_type=MESH).wait_send()


def solution(mesh):
    def local_fn(a_blk):
        cols = a_blk.shape[1]
        dma = pltpu.SemaphoreType.DMA
        out = pl.pallas_call(
            kernel,
            out_shape=jax.ShapeDtypeStruct((3, QR, ROWS), jnp.float32),
            in_specs=[pl.BlockSpec(memory_space=pltpu.HBM)],
            out_specs=pl.BlockSpec(memory_space=pltpu.VMEM),
            scratch_shapes=[
                pltpu.VMEM((3, ROWS, cols), jnp.bfloat16),
                pltpu.VMEM((3 * ROWS, ROWS), jnp.float32),
                pltpu.VMEM((2, 3 * ROWS, ROWS), jnp.float32),
                pltpu.VMEM((QR, ROWS), jnp.float32),
                pltpu.VMEM((2, PACK, TILE), jnp.float32),
                pltpu.VMEM((2, PACK, TILE), jnp.float32),
                dma((2,)), dma, dma((2, NZ)), dma, dma((NRECV,)), dma, dma((2,)), dma, dma,
            ],
            compiler_params=pltpu.CompilerParams(
                collective_id=0, has_side_effects=True, vmem_limit_bytes=50 * 2**20),
        )(a_blk)
        return out[None]

    return jax.shard_map(local_fn, mesh=mesh, in_specs=(P(("m", "g"), "kk"),),
                         out_specs=P(("m", "g"), None, "kk", None), check_vma=False)
```
